32 devices in a mesh: groups: 2 (over y), seq: 4 (over z), slide: 2 (over x), head: 2 (over core).
Axes of the slice: x: 2, y: 2, z: 4, core: 2. Of those that a mesh axis runs over, the one named last changes fastest.
Arguments:
- latents: bfloat16 [1024, 1024], P(('groups', 'seq'), 'head'), parts along dimension 0, may hold values from -153 to 153
- tile_keys: bfloat16 [4, 1024, 1024], P(('groups', 'slide'), 'seq', 'head'), parts along dimension 0, may hold values from -6 to 6
- tile_values: bfloat16 [4, 1024, 1024], P(('groups', 'slide'), 'seq', 'head'), parts along dimension 0, may hold values from -24 to 24
- tile_mask: int32 [4, 8], P(('groups', 'slide'), 'seq'), parts along dimension 0, may hold values from 0 to 1, as said below
- latent_counts: int32 [4], P(('groups', 'slide')), parts along dimension 0, may hold values from 128 to 512
- out_weight: bfloat16 [1024, 1024], P('head'), may hold values from -0.1875 to 0.1875
- cotangent: bfloat16 [4, 512, 1024], P(('groups', 'slide'), 'seq'), parts along dimension 0, may hold values from -6 to 6
Outputs:
- pooled: bfloat16 [4, 512, 1024], P(('groups', 'slide'), 'seq', 'head'), parts along dimension 0
- grad_latents: float32 [1024, 1024], P(('groups', 'seq'), 'head'), parts along dimension 0
- grad_keys: bfloat16 [4, 1024, 1024], P(('groups', 'slide'), 'seq', 'head'), parts along dimension 0
- grad_values: bfloat16 [4, 1024, 1024], P(('groups', 'slide'), 'seq', 'head'), parts along dimension 0
The draws below stay inside these ranges and needn't reach their ends.
There are 2 independent parts, one for each index of `groups`. The reference program is written for one: setup_inputs(seed, part) draws one part's arguments, and reference() takes and returns one part's arrays. A program takes and returns all parts, laid end to end along the dimension named above; an argument that names none is the same for every part. Nothing has to cross between parts.
Inputs may be any that keep to these rules, and one draw needn't show every extreme that they name: `tile_mask`: every slide has at least one block of 128 tiles marked 1.
All inputs are finite; a program needn't handle non-finite values.
Results may differ from the reference program's by a relative error of at most 0.035.
Values may be sent and summed in bfloat16 or wider, within the bound.
No kernel may reach another device: no remote copies, remote signals or barrier semaphores. Data moves between devices by JAX's collectives and lax.ppermute only.
A program may use at most 64 MiB of HBM per device.

```python
import jax
import jax.numpy as jnp
from jax import lax

D = 1024
H = 16
HD = 64
LAT = 512
BLOCK = 128
TILES = 1024
SLIDES = 2


def forced_blocks(key):
    return jax.random.randint(jax.random.fold_in(key, 11), (SLIDES,), 0, TILES // BLOCK)


def draw_tile_mask(key, part):
    drawn = jax.random.fold_in(key, 3)
    keep_rates = jax.random.randint(jax.random.fold_in(drawn, 1), (SLIDES, 1), 1, 8)
    block_rolls = jax.random.randint(jax.random.fold_in(drawn, 2), (SLIDES, TILES // BLOCK), 0, 8)
    blocks = (block_rolls < keep_rates).astype(jnp.int32)
    block_ids = jnp.arange(TILES // BLOCK)[None, :]
    forced_ids = forced_blocks(key)
    return jnp.where(block_ids == forced_ids[:, None], 1, blocks).astype(jnp.int32)


def draw_tile_keys(key, part):
    drawn = jax.random.normal(jax.random.fold_in(key, 5), (SLIDES, TILES, D), jnp.float32)
    return jnp.clip(drawn, -6.0, 6.0).astype(jnp.bfloat16)


def draw_latents(key, part):
    drawn = jax.random.normal(jax.random.fold_in(key, 9), (LAT, D), jnp.float32) * 2.5
    return jnp.clip(drawn, -15.0, 15.0).astype(jnp.bfloat16)


def levels(rng, extent, shards, least, largest):
    factor_of, own = 1.0, jax.random.fold_in(rng, 6)
    for dim, parts in shards:
        steps = jnp.exp(jax.random.uniform(jax.random.fold_in(own, dim), (parts,), jnp.float32, least / len(shards), largest / len(shards)))
        factor_of = factor_of * jnp.repeat(steps, extent[dim] // parts).reshape([-1 if axis == dim else 1 for axis in range(len(extent))])
    return factor_of


def bell_draw(rng, shape, deviation, bound, cuts=(), dtype=jnp.bfloat16):
    array = deviation * jax.random.normal(rng, shape, jnp.float32)
    if cuts:
        array = array * levels(rng, shape, cuts, -0.22, 0.18)
    return jnp.clip(array, -bound, bound).astype(dtype)


def setup_inputs(seed: int = 0, part: int = 0) -> dict:
    keys = jax.random.split(jax.random.key(seed), 8)
    own_keys = jax.random.split(jax.random.fold_in(keys[7], part), 8)
    return {
        "latents": draw_latents(jax.random.fold_in(jax.random.fold_in(keys[7], part), 71), part),
        "tile_keys": draw_tile_keys(jax.random.fold_in(jax.random.fold_in(keys[7], part), 71), part),
        "tile_values": bell_draw(own_keys[2], (SLIDES, TILES, D), 4.0, 24.0, ((0, 2), (1, 4), (2, 2))),
        "tile_mask": draw_tile_mask(jax.random.fold_in(jax.random.fold_in(keys[7], part), 71), part),
        "latent_counts": jax.random.randint(own_keys[4], (SLIDES,), LAT // 4, LAT + 1).astype(jnp.int32),
        "out_weight": bell_draw(keys[5], (D, D), D ** -0.5, 0.1875, ((0, 2),)),
        "cotangent": bell_draw(own_keys[6], (SLIDES, LAT, D), 1.0, 6.0, ((0, 2), (1, 4))),
    }


masked_score = -1.0e30


def reference(latents, tile_keys, tile_values, tile_mask, latent_counts, out_weight, cotangent):
    factor = HD ** -0.5
    query_heads = latents.reshape(LAT, H, HD).transpose(1, 0, 2)
    row_ids = jnp.arange(LAT).astype(jnp.int32)[:, None]

    def per_slide(inputs):
        key_block, value_block, blocks, live_count, slide_cot = inputs
        valid_tiles = jnp.repeat(blocks > 0, BLOCK)[None, :]
        key_heads = key_block.reshape(TILES, H, HD).transpose(1, 0, 2)
        value_heads = value_block.reshape(TILES, H, HD).transpose(1, 0, 2)

        def scored(query_h, key_h):
            raw_scores = jnp.dot(query_h, key_h.T, preferred_element_type=jnp.float32) * factor
            return jnp.where(valid_tiles, raw_scores, masked_score)

        def forward_head(pieces):
            query_h, key_h, value_h = pieces
            scores = scored(query_h, key_h)
            row_top = jnp.max(scores, axis=1, keepdims=True)
            expos = jnp.where(valid_tiles, jnp.exp(scores - row_top), 0.0)
            row_total = jnp.sum(expos, axis=1, keepdims=True)
            weighted = jnp.dot(expos.astype(jnp.bfloat16), value_h, preferred_element_type=jnp.float32)
            return weighted / row_total, row_top, row_total

        attn_heads, tops, totals = lax.map(forward_head, (query_heads, key_heads, value_heads))
        live = row_ids < live_count
        attended = jnp.where(live, attn_heads.transpose(1, 0, 2).reshape(LAT, D), 0.0).astype(jnp.bfloat16)
        pooled = jnp.dot(attended, out_weight, preferred_element_type=jnp.float32).astype(jnp.bfloat16)
        upstream = jnp.where(live, jnp.dot(slide_cot, out_weight.T, preferred_element_type=jnp.float32), 0.0).astype(jnp.bfloat16)
        up_heads = upstream.reshape(LAT, H, HD).transpose(1, 0, 2)
        att_heads = attended.reshape(LAT, H, HD).transpose(1, 0, 2)

        def backward_head(pieces):
            query_h, key_h, value_h, row_top, row_total, up_h, att_h = pieces
            row_delta = jnp.sum(up_h.astype(jnp.float32) * att_h.astype(jnp.float32), axis=1, keepdims=True)
            scores = scored(query_h, key_h)
            weights = jnp.where(valid_tiles, jnp.exp(scores - row_top), 0.0) / row_total
            grad_value = jnp.dot(weights.astype(jnp.bfloat16).T, up_h, preferred_element_type=jnp.float32)
            grad_prob = jnp.dot(up_h, value_h.T, preferred_element_type=jnp.float32)
            grad_score = (weights * (grad_prob - row_delta) * factor).astype(jnp.bfloat16)
            grad_query = jnp.dot(grad_score, key_h, preferred_element_type=jnp.float32)
            grad_key = jnp.dot(grad_score.T, query_h, preferred_element_type=jnp.float32)
            return grad_query, grad_key, grad_value

        grad_query, grad_key, grad_value = lax.map(backward_head, (query_heads, key_heads, value_heads, tops, totals, up_heads, att_heads))
        grad_query = grad_query.transpose(1, 0, 2).reshape(LAT, D)
        grad_key = grad_key.transpose(1, 0, 2).reshape(TILES, D).astype(jnp.bfloat16)
        grad_value = grad_value.transpose(1, 0, 2).reshape(TILES, D).astype(jnp.bfloat16)
        return pooled, grad_query, grad_key, grad_value

    pooled, grad_query, grad_keys, grad_values = lax.map(per_slide, (tile_keys, tile_values, tile_mask, latent_counts, cotangent))
    return pooled, jnp.sum(grad_query, axis=0), grad_keys, grad_values
```

```python
import functools
import math

import jax
import jax.numpy as jnp
from jax import lax
from jax.experimental import pallas as pl
from jax.experimental.pallas import tpu as pltpu
from jax.sharding import PartitionSpec as P

HD = 64
BLOCK = 128
LANES = 128
MASK_ROWS = 16

masked_score = -1e30


bf16 = jnp.bfloat16
f32 = jnp.float32


def gathered_body(latents, tile_keys, tile_values, tile_mask, latent_counts, out_weight, cotangent):
    local_rows = latents.shape[0]
    local_width = latents.shape[1]
    head_count = local_width // HD
    factor = HD ** (-0.5)
    queries = lax.all_gather(latents, "seq", axis=0, tiled=True)
    total_rows = queries.shape[0]
    first_row = lax.axis_index("seq") * local_rows
    every_row = lax.broadcasted_iota(jnp.int32, (total_rows, 1), 0)
    own_row = lax.broadcasted_iota(jnp.int32, (local_rows, 1), 0) + first_row
    tile_count = tile_keys.shape[1]
    key_block = tile_keys[0]
    value_block = tile_values[0]
    valid_tiles = jnp.broadcast_to(tile_mask[0][:, None] > 0, (tile_count // BLOCK, BLOCK)).reshape(
        1, tile_count
    )
    live_count = latent_counts[0]
    score_list = []
    for which_head in range(head_count):
        columns = slice(which_head * HD, (which_head + 1) * HD)
        raw_scores = (
            jnp.einsum(
                "qc,tc->qt",
                queries[:, columns],
                key_block[:, columns],
                preferred_element_type=jnp.float32,
            )
            * factor
        )
        score_list.append(jnp.where(valid_tiles, raw_scores, masked_score))
    local_top = jnp.stack([jnp.max(scored, axis=1) for scored in score_list], axis=1)
    row_top = lax.pmax(local_top, "seq")
    expo_list = []
    weighted_list = []
    total_list = []
    for which_head in range(head_count):
        columns = slice(which_head * HD, (which_head + 1) * HD)
        expos = jnp.where(
            valid_tiles,
            jnp.exp(score_list[which_head] - row_top[:, which_head : which_head + 1]),
            0.0,
        )
        expo_list.append(expos)
        total_list.append(jnp.sum(expos, axis=1))
        weighted_list.append(
            jnp.dot(
                expos.astype(jnp.bfloat16),
                value_block[:, columns],
                preferred_element_type=jnp.float32,
            )
        )
    partial_sums = jnp.concatenate(weighted_list, axis=1)
    partial_totals = jnp.stack(total_list, axis=1)
    weighted, totals = lax.psum((partial_sums, partial_totals), "seq")
    span = weighted.shape[0]
    attended = jnp.where(
        every_row < live_count,
        (weighted.reshape(span, head_count, HD) / totals[:, :, None]).reshape(span, local_width),
        0.0,
    ).astype(jnp.bfloat16)
    own_attended = lax.dynamic_slice_in_dim(attended, first_row, local_rows, 0)
    pooled_part = jnp.dot(own_attended, out_weight, preferred_element_type=jnp.float32)
    pooled_parts = [
        lax.psum_scatter(pooled_part.astype(jnp.bfloat16), "head", scatter_dimension=1, tiled=True)
    ]
    projected = jnp.einsum(
        "rd,cd->rc", cotangent[0], out_weight, preferred_element_type=jnp.float32
    )
    upstream = jnp.where(own_row < live_count, projected, 0.0).astype(jnp.bfloat16)
    upstream_all = lax.all_gather(upstream, "seq", axis=0, tiled=True)
    row_delta = jnp.sum(
        (upstream_all.astype(jnp.float32) * attended.astype(jnp.float32)).reshape(
            total_rows, head_count, HD
        ),
        axis=2,
    )
    query_list = []
    key_list = []
    value_list = []
    for which_head in range(head_count):
        columns = slice(which_head * HD, (which_head + 1) * HD)
        up_head = upstream_all[:, columns]
        weights = expo_list[which_head] / totals[:, which_head : which_head + 1]
        value_list.append(
            jnp.einsum(
                "qt,qc->tc",
                weights.astype(jnp.bfloat16),
                up_head,
                preferred_element_type=jnp.float32,
            )
        )
        grad_prob = jnp.einsum(
            "qc,tc->qt", up_head, value_block[:, columns], preferred_element_type=jnp.float32
        )
        grad_score = (
            weights * (grad_prob - row_delta[:, which_head : which_head + 1]) * factor
        ).astype(jnp.bfloat16)
        query_list.append(
            jnp.dot(grad_score, key_block[:, columns], preferred_element_type=jnp.float32)
        )
        key_list.append(
            jnp.einsum(
                "qt,qc->tc", grad_score, queries[:, columns], preferred_element_type=jnp.float32
            )
        )
    grad_rows = jnp.concatenate(query_list, axis=1)
    key_grads = [jnp.concatenate(key_list, axis=1).astype(jnp.bfloat16)]
    value_grads = [jnp.concatenate(value_list, axis=1).astype(jnp.bfloat16)]
    own_grad = lax.psum_scatter(
        grad_rows.astype(jnp.bfloat16), "seq", scatter_dimension=0, tiled=True
    )
    grad_latents = lax.psum(own_grad, "slide").astype(jnp.float32)
    return (
        jnp.stack(pooled_parts, axis=0),
        grad_latents,
        jnp.stack(key_grads, axis=0),
        jnp.stack(value_grads, axis=0),
    )


def dot_nn(a, b):
    return lax.dot_general(a, b, (((1,), (0,)), ((), ())), preferred_element_type=f32)


def dot_nt(a, b):
    return lax.dot_general(a, b, (((1,), (1,)), ((), ())), preferred_element_type=f32)


def lane_block(index, width):
    return pl.ds(pl.multiple_of(index * width, width), width)


def pack_keys_kernel(n, place_ref, mask_ref, keys_ref, latents_ref, *outs):
    me = place_ref[0]
    tiles, rows, width = keys_ref.shape[1], latents_ref.shape[0], outs[0].shape[1]
    row_id = lax.broadcasted_iota(jnp.int32, (MASK_ROWS, width), 0)
    flags = jnp.zeros((MASK_ROWS, width), f32)
    for block in range(tiles // BLOCK):
        value = jnp.where(mask_ref[0, block] > 0, 1.0, 0.0)
        flags = jnp.where(row_id == block, value, flags)
    for d in range(n):
        columns = lane_block(lax.rem(me + d, n), width)
        outs[d][:tiles, :] = keys_ref[0, :, columns]
        outs[d][tiles : tiles + rows, :] = latents_ref[:, columns]
        outs[d][tiles + rows :, :] = flags.astype(bf16)


def pack_values_kernel(n, place_ref, count_ref, values_ref, weight_ref, cot_ref, *rest):
    outs, up_ref = rest[:n], rest[n]
    me = place_ref[0]
    tiles, width = values_ref.shape[1], outs[0].shape[1]
    rows = cot_ref.shape[1]
    row_id = lax.broadcasted_iota(jnp.int32, (1, rows), 1) + me * rows
    live = row_id < count_ref[0]
    projected = dot_nt(weight_ref[...], cot_ref[0])
    up_ref[...] = jnp.where(live, projected, 0.0).astype(bf16)
    for d in range(n):
        owner = lax.rem(me + d, n)
        outs[d][:width, :] = up_ref[lane_block(owner, width), :]
        outs[d][width:, :] = values_ref[0, :, lane_block(owner, width)]


def attend_kernel(n, heads, place_ref, count_ref, *refs):
    a_refs, b_refs = refs[:n], refs[n : 2 * n]
    c_refs, k_refs = refs[2 * n : 3 * n], refs[3 * n : 4 * n]
    query_grad_ref = refs[4 * n]
    score_ref, expo_ref = refs[4 * n + 1], refs[4 * n + 2]
    me = place_ref[0]
    width = heads * HD
    rows = b_refs[0].shape[1]
    tiles = b_refs[0].shape[0] - width
    total_rows = n * rows
    per_block = tiles // BLOCK
    factor = HD ** (-0.5)
    scale = factor * math.log2(math.e)

    queries = jnp.concatenate([a_refs[d][tiles : tiles + rows, :] for d in range(n)], axis=0)
    queries_t = queries.astype(f32).T.astype(bf16)
    upstream_t = jnp.concatenate([b_refs[d][:width, :] for d in range(n)], axis=1)
    head_of_row = lax.broadcasted_iota(jnp.int32, (width, total_rows), 0) // HD
    head_of_lane = lax.broadcasted_iota(jnp.int32, (total_rows, width), 1) // HD
    lane_row = lax.broadcasted_iota(jnp.int32, (1, rows), 1)
    live = jnp.concatenate(
        [lane_row + lax.rem(me + n - d, n) * rows < count_ref[0] for d in range(n)], axis=1
    )
    valid = []
    for d in range(n):
        for j in range(per_block):
            flag = a_refs[d][tiles + rows : tiles + rows + MASK_ROWS, :].astype(f32)[j : j + 1, :]
            valid.append(jnp.concatenate([flag] * (total_rows // width), axis=1) > 0.5)

    values_t = [b_refs[d][width:, :].astype(f32).T.astype(bf16) for d in range(n)]
    keys_t = [a_refs[d][:tiles, :].astype(f32).T.astype(bf16) for d in range(n)]
    gained = []
    attended_list = []
    delta_list = []
    for h in range(heads):
        own_rows = slice(h * HD, (h + 1) * HD)
        top = jnp.full((1, total_rows), masked_score, f32)
        query_h = jnp.where(head_of_row == h, queries_t, jnp.zeros_like(queries_t))
        for d in range(n):
            scored = dot_nn(a_refs[d][:tiles, :], query_h) * scale
            score_ref[d] = scored
            for j in range(per_block):
                block_top = jnp.max(scored[j * BLOCK : (j + 1) * BLOCK], axis=0, keepdims=True)
                top = jnp.maximum(top, jnp.where(valid[d * per_block + j], block_top, masked_score))
        total = jnp.zeros((1, total_rows), f32)
        weighted = jnp.zeros((HD, total_rows), f32)
        for d in range(n):
            for j in range(per_block):
                part = slice(j * BLOCK, (j + 1) * BLOCK)
                expos = jnp.where(
                    valid[d * per_block + j], jnp.exp2(score_ref[d, part, :] - top), 0.0
                )
                total = total + jnp.sum(expos, axis=0, keepdims=True)
                expo_ref[h, d, part, :] = expos.astype(bf16)
            weighted = weighted + dot_nn(values_t[d][own_rows, :], expo_ref[h, d])
        inverse = 1.0 / total
        attended_h = jnp.where(live, weighted * inverse, 0.0).astype(bf16)
        up_h = (upstream_t[own_rows, :].astype(f32) * (inverse * factor)).astype(bf16)
        delta_list.append(
            jnp.sum(up_h.astype(f32) * attended_h.astype(f32), axis=0, keepdims=True)
        )
        attended_list.append(attended_h)
        gained.append(up_h)
    attended = jnp.concatenate(attended_list, axis=0)
    up_scaled_t = jnp.concatenate(gained, axis=0)
    up_scaled = up_scaled_t.astype(f32).T.astype(bf16)
    zero_rows = jnp.zeros_like(up_scaled)
    zero_cols = jnp.zeros_like(up_scaled_t)
    up_heads = [jnp.where(head_of_lane == h, up_scaled, zero_rows) for h in range(heads)]
    query_heads = [jnp.where(head_of_lane == h, queries, zero_rows) for h in range(heads)]
    up_heads_t = [jnp.where(head_of_row == h, up_scaled_t, zero_cols) for h in range(heads)]
    query_grad = [jnp.zeros((HD, total_rows), f32) for _ in range(heads)]
    for d in range(n):
        value_grad = jnp.zeros((tiles, width), f32)
        key_grad = jnp.zeros((tiles, width), f32)
        for h in range(heads):
            expos = expo_ref[h, d]
            value_grad = value_grad + dot_nn(expos, up_heads[h])
            grad_prob = dot_nn(b_refs[d][width:, :], up_heads_t[h])
            grad_score = (expos.astype(f32) * (grad_prob - delta_list[h])).astype(bf16)
            key_grad = key_grad + dot_nn(grad_score, query_heads[h])
            query_grad[h] = query_grad[h] + dot_nn(
                keys_t[d][h * HD : (h + 1) * HD, :], grad_score
            )
        c_refs[d][:tiles, :] = (value_grad * (1.0 / factor)).astype(bf16)
        c_refs[d][tiles:, :] = attended[:, d * rows : (d + 1) * rows]
        k_refs[d][...] = key_grad.astype(bf16)
    query_grad_ref[...] = jnp.concatenate(query_grad, axis=0).astype(bf16)


def values_home_kernel(n, place_ref, weight_ref, *refs):
    c_refs = refs[:n]
    value_grad_ref, kept_ref, sent_ref = refs[n : n + 3]
    me, side = place_ref[0], place_ref[1]
    width = c_refs[0].shape[1]
    tiles = value_grad_ref.shape[1]
    half = kept_ref.shape[1]
    kept = jnp.zeros(kept_ref.shape, f32)
    sent = jnp.zeros(sent_ref.shape, f32)
    for d in range(n):
        owner = lax.rem(me + d, n)
        value_grad_ref[0, :, lane_block(owner, width)] = c_refs[d][:tiles, :]
        attended = c_refs[d][tiles:, :].astype(f32).T.astype(bf16)
        inputs = lane_block(owner, width)
        kept = kept + dot_nn(attended, weight_ref[inputs, lane_block(side, half)])
        sent = sent + dot_nn(attended, weight_ref[inputs, lane_block(1 - side, half)])
    kept_ref[...] = kept
    sent_ref[...] = sent.astype(bf16)


def join_kernel(n, *refs):
    own_ref, other_ref = refs[0], refs[1]
    k_refs, e_refs = refs[2 : 2 + n], refs[2 + n :]
    tiles, rows = k_refs[0].shape[0], e_refs[0].shape[1]
    both = (own_ref[...].astype(f32) + other_ref[...].astype(f32)).astype(bf16)
    for d in range(n):
        e_refs[d][:tiles, :] = k_refs[d][...]
        e_refs[d][tiles:, :] = both[:, d * rows : (d + 1) * rows]


def keys_home_kernel(n, place_ref, *refs):
    e_refs = refs[:n]
    key_grad_ref, latent_grad_ref = refs[n : n + 2]
    me = place_ref[0]
    width = e_refs[0].shape[1]
    tiles = key_grad_ref.shape[1]
    for d in range(n):
        columns = lane_block(lax.rem(me + d, n), width)
        key_grad_ref[0, :, columns] = e_refs[d][:tiles, :]
        latent_grad_ref[:, columns] = e_refs[d][tiles:, :].astype(f32).T


SMEM = pl.BlockSpec(memory_space=pltpu.SMEM)
VMEM = pl.BlockSpec(memory_space=pltpu.VMEM)


def call(kernel, out_shape, smem, vmem, flops, name, scratch=()):
    moved = sum(x.size * x.dtype.itemsize for x in vmem)
    moved += sum(math.prod(x.shape) * x.dtype.itemsize for x in out_shape)
    return pl.pallas_call(
        kernel,
        out_shape=out_shape,
        in_specs=[SMEM] * len(smem) + [VMEM] * len(vmem),
        out_specs=[VMEM] * len(out_shape),
        scratch_shapes=list(scratch),
        cost_estimate=pl.CostEstimate(flops=int(flops), bytes_accessed=moved, transcendentals=0),
        name=name,
    )(*smem, *vmem)


def exchanged_body(n, sides, latents, tile_keys, tile_values, tile_mask, latent_counts, out_weight, cotangent):
    rows, local_width = latents.shape
    tiles = tile_keys.shape[1]
    out_width = out_weight.shape[1]
    heads = local_width // HD // n
    width = heads * HD
    total_rows = n * rows
    place = jnp.stack([lax.axis_index("seq"), lax.axis_index("head")]).astype(jnp.int32)
    sds = jax.ShapeDtypeStruct

    def shift(x, d):
        return lax.ppermute(x, "seq", [(i, (i + d) % n) for i in range(n)])

    packed_keys = call(
        functools.partial(pack_keys_kernel, n),
        [sds((tiles + rows + MASK_ROWS, width), bf16)] * n,
        (place, tile_mask),
        (tile_keys, latents),
        1e6,
        "pack_keys",
    )
    a_list = [packed_keys[0]] + [shift(packed_keys[d], d) for d in range(1, n)]
    packed_values = call(
        functools.partial(pack_values_kernel, n),
        [sds((width + tiles, width), bf16)] * n,
        (place, latent_counts),
        (tile_values, out_weight, cotangent),
        2 * rows * local_width * out_width,
        "pack_values",
        [pltpu.VMEM((local_width, rows), bf16)],
    )
    b_list = [packed_values[0]] + [shift(packed_values[d], d) for d in range(1, n)]
    outs = call(
        functools.partial(attend_kernel, n, heads),
        [sds((tiles + width, width), bf16)] * n
        + [sds((tiles, width), bf16)] * n
        + [sds((width, total_rows), bf16)],
        (place, latent_counts),
        (*a_list, *b_list),
        12 * total_rows * n * tiles * width,
        "attend",
        [
            pltpu.VMEM((n, tiles, total_rows), f32),
            pltpu.VMEM((heads, n, tiles, total_rows), bf16),
        ],
    )
    c_out, k_out, query_grad = outs[:n], outs[n : 2 * n], outs[2 * n]
    other_grad = query_grad
    c_list = [c_out[0]] + [shift(c_out[d], n - d) for d in range(1, n)]
    others = []
    for step in range(1, sides):
        others.append(
            lax.ppermute(other_grad, "slide", [(i, (i + step) % sides) for i in range(sides)])
        )
    other_sum = others[0]
    for more in others[1:]:
        other_sum = other_sum.astype(f32) + more.astype(f32)
    joined = call(
        functools.partial(join_kernel, n),
        [sds((tiles + width, width), bf16)] * n,
        (),
        (query_grad, other_sum, *k_out),
        1e6,
        "join",
    )
    e_list = [joined[0]] + [shift(joined[d], n - d) for d in range(1, n)]
    value_grads, kept, sent = call(
        functools.partial(values_home_kernel, n),
        [
            sds(tile_values.shape, bf16),
            sds((rows, out_width // 2), f32),
            sds((rows, out_width // 2), bf16),
        ],
        (place,),
        (out_weight, *c_list),
        2 * rows * local_width * out_width,
        "values_home",
    )
    came = lax.ppermute(sent, "head", [(0, 1), (1, 0)])
    pooled = (kept + came.astype(f32)).astype(bf16)[None]
    key_grads, latent_grads = call(
        functools.partial(keys_home_kernel, n),
        [sds(tile_keys.shape, bf16), sds(latents.shape, f32)],
        (place,),
        tuple(e_list),
        1e6,
        "keys_home",
    )
    return pooled, latent_grads, key_grads, value_grads


def solution(mesh):
    placed = (
        P(("groups", "seq"), "head"),
        P(("groups", "slide"), "seq", "head"),
        P(("groups", "slide"), "seq", "head"),
        P(("groups", "slide"), "seq"),
        P(("groups", "slide")),
        P("head", None),
        P(("groups", "slide"), "seq", None),
    )
    n, sides = mesh.shape["seq"], mesh.shape["slide"]

    def body(latents, tile_keys, *rest):
        rows, local_width = latents.shape
        tiles = tile_keys.shape[1]
        fits = (
            mesh.shape["head"] == 2
            and sides > 1
            and local_width % (n * LANES) == 0
            and local_width // n == rows
            and tiles % BLOCK == 0
            and tiles // BLOCK <= MASK_ROWS
        )
        if fits:
            return exchanged_body(n, sides, latents, tile_keys, *rest)
        return gathered_body(latents, tile_keys, *rest)

    return jax.shard_map(
        body,
        mesh=mesh,
        in_specs=placed,
        out_specs=(
            P(("groups", "slide"), "seq", "head"),
            P(("groups", "seq"), "head"),
            P(("groups", "slide"), "seq", "head"),
            P(("groups", "slide"), "seq", "head"),
        ),
        check_vma=False,
    )
```

```python
import functools
import math

import jax
import jax.numpy as jnp
from jax import lax
from jax.experimental import pallas as pl
from jax.experimental.pallas import tpu as pltpu
from jax.sharding import PartitionSpec as P


HD = 64
BLOCK = 128
LANES = 128
MASK_ROWS = 16

masked_score = -1e30


bf16 = jnp.bfloat16
f32 = jnp.float32


def gathered_body(latents, tile_keys, tile_values, tile_mask, latent_counts, out_weight, cotangent):
    local_rows = latents.shape[0]
    local_width = latents.shape[1]
    head_count = local_width // HD
    factor = HD ** (-0.5)
    queries = lax.all_gather(latents, "seq", axis=0, tiled=True)
    total_rows = queries.shape[0]
    first_row = lax.axis_index("seq") * local_rows
    every_row = lax.broadcasted_iota(jnp.int32, (total_rows, 1), 0)
    own_row = lax.broadcasted_iota(jnp.int32, (local_rows, 1), 0) + first_row
    tile_count = tile_keys.shape[1]
    key_block = tile_keys[0]
    value_block = tile_values[0]
    valid_tiles = jnp.broadcast_to(tile_mask[0][:, None] > 0, (tile_count // BLOCK, BLOCK)).reshape(
        1, tile_count
    )
    live_count = latent_counts[0]
    score_list = []
    for which_head in range(head_count):
        columns = slice(which_head * HD, (which_head + 1) * HD)
        raw_scores = (
            jnp.einsum(
                "qc,tc->qt",
                queries[:, columns],
                key_block[:, columns],
                preferred_element_type=jnp.float32,
            )
            * factor
        )
        score_list.append(jnp.where(valid_tiles, raw_scores, masked_score))
    local_top = jnp.stack([jnp.max(scored, axis=1) for scored in score_list], axis=1)
    row_top = lax.pmax(local_top, "seq")
    expo_list = []
    weighted_list = []
    total_list = []
    for which_head in range(head_count):
        columns = slice(which_head * HD, (which_head + 1) * HD)
        expos = jnp.where(
            valid_tiles,
            jnp.exp(score_list[which_head] - row_top[:, which_head : which_head + 1]),
            0.0,
        )
        expo_list.append(expos)
        total_list.append(jnp.sum(expos, axis=1))
        weighted_list.append(
            jnp.dot(
                expos.astype(jnp.bfloat16),
                value_block[:, columns],
                preferred_element_type=jnp.float32,
            )
        )
    partial_sums = jnp.concatenate(weighted_list, axis=1)
    partial_totals = jnp.stack(total_list, axis=1)
    weighted, totals = lax.psum((partial_sums, partial_totals), "seq")
    span = weighted.shape[0]
    attended = jnp.where(
        every_row < live_count,
        (weighted.reshape(span, head_count, HD) / totals[:, :, None]).reshape(span, local_width),
        0.0,
    ).astype(jnp.bfloat16)
    own_attended = lax.dynamic_slice_in_dim(attended, first_row, local_rows, 0)
    pooled_part = jnp.dot(own_attended, out_weight, preferred_element_type=jnp.float32)
    pooled_parts = [
        lax.psum_scatter(pooled_part.astype(jnp.bfloat16), "head", scatter_dimension=1, tiled=True)
    ]
    projected = jnp.einsum(
        "rd,cd->rc", cotangent[0], out_weight, preferred_element_type=jnp.float32
    )
    upstream = jnp.where(own_row < live_count, projected, 0.0).astype(jnp.bfloat16)
    upstream_all = lax.all_gather(upstream, "seq", axis=0, tiled=True)
    row_delta = jnp.sum(
        (upstream_all.astype(jnp.float32) * attended.astype(jnp.float32)).reshape(
            total_rows, head_count, HD
        ),
        axis=2,
    )
    query_list = []
    key_list = []
    value_list = []
    for which_head in range(head_count):
        columns = slice(which_head * HD, (which_head + 1) * HD)
        up_head = upstream_all[:, columns]
        weights = expo_list[which_head] / totals[:, which_head : which_head + 1]
        value_list.append(
            jnp.einsum(
                "qt,qc->tc",
                weights.astype(jnp.bfloat16),
                up_head,
                preferred_element_type=jnp.float32,
            )
        )
        grad_prob = jnp.einsum(
            "qc,tc->qt", up_head, value_block[:, columns], preferred_element_type=jnp.float32
        )
        grad_score = (
            weights * (grad_prob - row_delta[:, which_head : which_head + 1]) * factor
        ).astype(jnp.bfloat16)
        query_list.append(
            jnp.dot(grad_score, key_block[:, columns], preferred_element_type=jnp.float32)
        )
        key_list.append(
            jnp.einsum(
                "qt,qc->tc", grad_score, queries[:, columns], preferred_element_type=jnp.float32
            )
        )
    grad_rows = jnp.concatenate(query_list, axis=1)
    key_grads = [jnp.concatenate(key_list, axis=1).astype(jnp.bfloat16)]
    value_grads = [jnp.concatenate(value_list, axis=1).astype(jnp.bfloat16)]
    own_grad = lax.psum_scatter(
        grad_rows.astype(jnp.bfloat16), "seq", scatter_dimension=0, tiled=True
    )
    grad_latents = lax.psum(own_grad, "slide").astype(jnp.float32)
    return (
        jnp.stack(pooled_parts, axis=0),
        grad_latents,
        jnp.stack(key_grads, axis=0),
        jnp.stack(value_grads, axis=0),
    )


def dot_nn(a, b):
    return lax.dot_general(a, b, (((1,), (0,)), ((), ())), preferred_element_type=f32)


def dot_nt(a, b):
    return lax.dot_general(a, b, (((1,), (1,)), ((), ())), preferred_element_type=f32)


def lane_block(index, width):
    return pl.ds(pl.multiple_of(index * width, width), width)


def pack_kernel(n, count_ref, mask_ref, keys_ref, latents_ref, values_ref, weight_ref, cot_ref, *rest):
    a_outs, v_outs, live_ref = rest[:n], rest[n : 2 * n], rest[2 * n]
    mask, weight, cot, up_ref, sems = rest[2 * n + 1 :]
    me = lax.axis_index("seq")
    tiles, width = v_outs[0].shape
    rows = cot.shape[0]
    sources = [
        (mask_ref, mask),
        (weight_ref, weight),
        (cot_ref.at[0], cot),
    ]
    for d in range(n):
        columns = lane_block(lax.rem(me + d, n), width)
        sources.append((keys_ref.at[0, :, columns], a_outs[d].at[:tiles, :]))
        sources.append((latents_ref.at[:, columns], a_outs[d].at[tiles : tiles + rows, :]))
        sources.append((values_ref.at[0, :, columns], v_outs[d]))
    copies = [
        pltpu.make_async_copy(source, target, sems.at[i])
        for i, (source, target) in enumerate(sources)
    ]
    for copy in copies:
        copy.start()
    for copy in copies[:3]:
        copy.wait()
    row_id = lax.broadcasted_iota(jnp.int32, (MASK_ROWS, width), 0)
    flags = jnp.zeros((MASK_ROWS, width), f32)
    for block in range(tiles // BLOCK):
        value = jnp.where(mask[0, block] > 0, 1.0, 0.0)
        flags = jnp.where(row_id == block, value, flags)
    lane_row = lax.broadcasted_iota(jnp.int32, (1, rows), 1)
    projected = dot_nt(weight[...], cot[...])
    up_ref[...] = jnp.where(lane_row + me * rows < count_ref[0], projected, 0.0).astype(bf16)
    for d in range(n):
        owner = lax.rem(me + d, n)
        a_outs[d][tiles + rows : tiles + rows + width, :] = up_ref[lane_block(owner, width), :]
        a_outs[d][tiles + rows + width :, :] = flags.astype(bf16)
        source_row = lane_row + lax.rem(me + n - d, n) * rows
        live_ref[:, d * rows : (d + 1) * rows] = jnp.where(source_row < count_ref[0], 1.0, 0.0)
    for copy in copies[3:]:
        copy.wait()


def head_mask(h, shape, axis):
    return lax.broadcasted_iota(jnp.int32, shape, axis) // HD == h


def softmax_kernel(n, heads, rows, *refs):
    a_refs = refs[:n]
    expo_ref, total_ref, keys_t_ref, score_ref = refs[n:]
    width = heads * HD
    tiles = expo_ref.shape[2]
    total_rows = n * rows
    per_block = tiles // BLOCK
    scale = HD ** (-0.5) * math.log2(math.e)
    queries = jnp.concatenate([a_refs[d][tiles : tiles + rows, :] for d in range(n)], axis=0)
    queries_t = queries.astype(f32).T.astype(bf16)
    valid = []
    for d in range(n):
        flags = a_refs[d][tiles + rows + width :, :].astype(f32)
        for j in range(per_block):
            valid.append(
                jnp.concatenate([flags[j : j + 1, :]] * (total_rows // width), axis=1) > 0.5
            )
    for h in range(heads):
        top = jnp.full((1, total_rows), masked_score, f32)
        query_h = jnp.where(
            head_mask(h, (width, total_rows), 0), queries_t, jnp.zeros_like(queries_t)
        )
        for d in range(n):
            scored = dot_nn(a_refs[d][:tiles, :], query_h)
            score_ref[d] = scored
            for j in range(per_block):
                block_top = jnp.max(scored[j * BLOCK : (j + 1) * BLOCK], axis=0, keepdims=True)
                top = jnp.maximum(top, jnp.where(valid[d * per_block + j], block_top, masked_score))
        total = jnp.zeros((1, total_rows), f32)
        for d in range(n):
            for j in range(per_block):
                part = slice(j * BLOCK, (j + 1) * BLOCK)
                expos = jnp.where(
                    valid[d * per_block + j], jnp.exp2((score_ref[d, part, :] - top) * scale), 0.0
                )
                total = total + jnp.sum(expos, axis=0, keepdims=True)
                expo_ref[h, d, part, :] = expos.astype(bf16)
        total_ref[h] = total
    for d in range(n):
        keys_t_ref[d] = a_refs[d][:tiles, :].astype(f32).T.astype(bf16)


def value_grads_kernel(n, heads, expo_ref, total_ref, *refs):
    a_refs, up_ref, outs = refs[:n], refs[n], refs[n + 1 :]
    factor = HD ** (-0.5)
    width = heads * HD
    first = a_refs[0].shape[0] - MASK_ROWS - width
    upstream_t = jnp.concatenate(
        [a_refs[d][first : first + width, :] for d in range(n)], axis=1
    )
    up_scaled_t = jnp.concatenate(
        [
            upstream_t[h * HD : (h + 1) * HD, :].astype(f32) * (factor / total_ref[h])
            for h in range(heads)
        ],
        axis=0,
    )
    up_ref[...] = up_scaled_t.astype(bf16)
    up_scaled = up_scaled_t.T
    up_heads = [
        jnp.where(head_mask(h, up_scaled.shape, 1), up_scaled, 0.0).astype(bf16)
        for h in range(heads)
    ]
    for d in range(n):
        value_grad = dot_nn(expo_ref[0, d], up_heads[0])
        for h in range(1, heads):
            value_grad = value_grad + dot_nn(expo_ref[h, d], up_heads[h])
        outs[d][...] = (value_grad * (1.0 / factor)).astype(bf16)


def key_grads_kernel(n, heads, rows, live_ref, expo_ref, total_ref, up_ref, keys_t_ref, *refs):
    a_refs, v_refs = refs[:n], refs[n : 2 * n]
    outs, query_grad_ref = refs[2 * n : 3 * n], refs[3 * n]
    width = heads * HD
    tiles = v_refs[0].shape[0]
    total_rows = n * rows
    live = live_ref[...] > 0.5
    queries = jnp.concatenate([a_refs[d][tiles : tiles + rows, :] for d in range(n)], axis=0)
    up_scaled_t = up_ref[...]
    values_t = [v_refs[d][...].astype(f32).T.astype(bf16) for d in range(n)]
    attended_list = []
    delta_list = []
    for h in range(heads):
        own_rows = slice(h * HD, (h + 1) * HD)
        weighted = dot_nn(values_t[0][own_rows, :], expo_ref[h, 0])
        for d in range(1, n):
            weighted = weighted + dot_nn(values_t[d][own_rows, :], expo_ref[h, d])
        attended_h = jnp.where(live, weighted / total_ref[h], 0.0).astype(bf16)
        delta_list.append(
            jnp.sum(
                up_scaled_t[own_rows, :].astype(f32) * attended_h.astype(f32),
                axis=0,
                keepdims=True,
            )
        )
        attended_list.append(attended_h)
    attended = jnp.concatenate(attended_list, axis=0)
    zero_rows = jnp.zeros_like(queries)
    zero_cols = jnp.zeros_like(up_scaled_t)
    query_heads = [jnp.where(head_mask(h, queries.shape, 1), queries, zero_rows) for h in range(heads)]
    up_heads_t = [
        jnp.where(head_mask(h, up_scaled_t.shape, 0), up_scaled_t, zero_cols) for h in range(heads)
    ]
    query_grad = [jnp.zeros((HD, total_rows), f32) for _ in range(heads)]
    for d in range(n):
        key_grad = jnp.zeros((tiles, width), f32)
        for h in range(heads):
            grad_prob = dot_nn(v_refs[d][...], up_heads_t[h])
            grad_score = (expo_ref[h, d].astype(f32) * (grad_prob - delta_list[h])).astype(bf16)
            key_grad = key_grad + dot_nn(grad_score, query_heads[h])
            query_grad[h] = query_grad[h] + dot_nn(
                keys_t_ref[d, h * HD : (h + 1) * HD, :], grad_score
            )
        outs[d][:tiles, :] = key_grad.astype(bf16)
        outs[d][tiles:, :] = attended[:, d * rows : (d + 1) * rows]
    query_grad_ref[...] = jnp.concatenate(query_grad, axis=0).astype(bf16)


def values_home_kernel(n, *refs):
    c_refs, value_grad_ref = refs[:n], refs[n]
    me = lax.axis_index("seq")
    width = c_refs[0].shape[1]
    for d in range(n):
        value_grad_ref[0, :, lane_block(lax.rem(me + d, n), width)] = c_refs[d][...]


def pool_kernel(n, weight_ref, *refs):
    k_refs = refs[:n]
    key_grad_ref, kept_ref, sent_ref = refs[n : n + 3]
    me, side = lax.axis_index("seq"), lax.axis_index("head")
    width = k_refs[0].shape[1]
    tiles = key_grad_ref.shape[1]
    half = kept_ref.shape[1]
    kept = jnp.zeros(kept_ref.shape, f32)
    sent = jnp.zeros(sent_ref.shape, f32)
    for d in range(n):
        owner = lax.rem(me + d, n)
        key_grad_ref[0, :, lane_block(owner, width)] = k_refs[d][:tiles, :]
        attended = k_refs[d][tiles:, :].astype(f32).T.astype(bf16)
        inputs = lane_block(owner, width)
        kept = kept + dot_nn(attended, weight_ref[inputs, lane_block(side, half)])
        sent = sent + dot_nn(attended, weight_ref[inputs, lane_block(1 - side, half)])
    kept_ref[...] = kept
    sent_ref[...] = sent.astype(bf16)


def join_kernel(n, own_ref, other_ref, *outs):
    rows = outs[0].shape[1]
    both = (own_ref[...].astype(f32) + other_ref[...].astype(f32)).astype(bf16)
    for d in range(n):
        outs[d][...] = both[:, d * rows : (d + 1) * rows]


def last_kernel(n, kept_ref, came_ref, *refs):
    g_refs, latent_grad_ref, pooled_ref = refs[:n], refs[n], refs[n + 1]
    me = lax.axis_index("seq")
    width = g_refs[0].shape[0]
    for d in range(n):
        columns = lane_block(lax.rem(me + d, n), width)
        latent_grad_ref[:, columns] = g_refs[d][...].astype(f32).T
    pooled_ref[0] = (kept_ref[...] + came_ref[...].astype(f32)).astype(bf16)


SMEM = pl.BlockSpec(memory_space=pltpu.SMEM)
HBM = pl.BlockSpec(memory_space=pltpu.HBM)
VMEM = pl.BlockSpec(memory_space=pltpu.VMEM)


def call(kernel, out_shape, operands, flops, scratch=(), grant=8, spaces=None):
    moved = sum(x.size * x.dtype.itemsize for x in operands)
    moved += sum(math.prod(x.shape) * x.dtype.itemsize for x in out_shape)
    return pl.pallas_call(
        kernel,
        out_shape=out_shape,
        in_specs=spaces or [VMEM] * len(operands),
        out_specs=[VMEM] * len(out_shape),
        scratch_shapes=list(scratch),
        cost_estimate=pl.CostEstimate(flops=int(flops), bytes_accessed=moved, transcendentals=0),
        compiler_params=pltpu.CompilerParams(vmem_limit_bytes=grant * 1024 * 1024),
    )(*operands)


def exchanged_body(n, sides, latents, tile_keys, tile_values, tile_mask, latent_counts, out_weight, cotangent):
    rows, local_width = latents.shape
    tiles = tile_keys.shape[1]
    out_width = out_weight.shape[1]
    heads = local_width // HD // n
    width = heads * HD
    total_rows = n * rows
    sds = jax.ShapeDtypeStruct
    product = 2 * total_rows * n * tiles * width

    def spread(pieces, sign):
        return [pieces[0]] + [
            lax.ppermute(pieces[d], "seq", [(i, (i + sign * d) % n) for i in range(n)])
            for d in range(1, n)
        ]

    *packed, live = call(
        functools.partial(pack_kernel, n),
        [sds((tiles + rows + width + MASK_ROWS, width), bf16)] * n
        + [sds((tiles, width), bf16)] * n
        + [sds((1, total_rows), f32)],
        (
            latent_counts,
            *(
                pltpu.with_memory_space_constraint(x, pltpu.HBM)
                for x in (tile_mask, tile_keys, latents, tile_values, out_weight, cotangent)
            ),
        ),
        2 * rows * local_width * out_width,
        [
            pltpu.SMEM(tile_mask.shape, jnp.int32),
            pltpu.VMEM(out_weight.shape, bf16),
            pltpu.VMEM(cotangent.shape[1:], bf16),
            pltpu.VMEM((local_width, rows), bf16),
            pltpu.SemaphoreType.DMA((3 + 3 * n,)),
        ],
        spaces=[SMEM] + [HBM] * 6,
    )
    a_list = spread(packed[:n], 1)
    v_list = spread(packed[n:], 1)
    expos, totals, keys_t = call(
        functools.partial(softmax_kernel, n, heads, rows),
        [
            sds((heads, n, tiles, total_rows), bf16),
            sds((heads, 1, total_rows), f32),
            sds((n, width, tiles), bf16),
        ],
        a_list,
        product,
        [pltpu.VMEM((n, tiles, total_rows), f32)],
        16,
    )
    up_scaled, *c_out = call(
        functools.partial(value_grads_kernel, n, heads),
        [sds((width, total_rows), bf16)] + [sds((tiles, width), bf16)] * n,
        (expos, totals, *a_list),
        product,
        (),
        16,
    )
    c_list = spread(c_out, -1)
    *k_out, query_grad = call(
        functools.partial(key_grads_kernel, n, heads, rows),
        [sds((tiles + width, width), bf16)] * n + [sds((width, total_rows), bf16)],
        (live, expos, totals, up_scaled, keys_t, *a_list, *v_list),
        4 * product,
        (),
        16,
    )
    other_sum = None
    for step in range(1, sides):
        came = lax.ppermute(query_grad, "slide", [(i, (i + step) % sides) for i in range(sides)])
        other_sum = came if other_sum is None else other_sum.astype(f32) + came.astype(f32)
    k_list = spread(k_out, -1)
    joined = call(
        functools.partial(join_kernel, n),
        [sds((width, rows), bf16)] * n,
        (query_grad, other_sum),
        1e6,
    )
    g_list = spread(joined, -1)
    (value_grads,) = call(
        functools.partial(values_home_kernel, n), [sds(tile_values.shape, bf16)], c_list, 1e6
    )
    key_grads, kept, sent = call(
        functools.partial(pool_kernel, n),
        [
            sds(tile_keys.shape, bf16),
            sds((rows, out_width // 2), f32),
            sds((rows, out_width // 2), bf16),
        ],
        (out_weight, *k_list),
        2 * rows * local_width * out_width,
    )
    came = lax.ppermute(sent, "head", [(0, 1), (1, 0)])
    latent_grads, pooled = call(
        functools.partial(last_kernel, n),
        [sds(latents.shape, f32), sds((1, rows, out_width // 2), bf16)],
        (kept, came, *g_list),
        1e6,
    )
    return pooled, latent_grads, key_grads, value_grads


def solution(mesh):
    placed = (
        P(("groups", "seq"), "head"),
        P(("groups", "slide"), "seq", "head"),
        P(("groups", "slide"), "seq", "head"),
        P(("groups", "slide"), "seq"),
        P(("groups", "slide")),
        P("head", None),
        P(("groups", "slide"), "seq", None),
    )
    n, sides = mesh.shape["seq"], mesh.shape["slide"]

    def body(latents, tile_keys, *rest):
        rows, local_width = latents.shape
        tiles = tile_keys.shape[1]
        fits = (
            mesh.shape["head"] == 2
            and sides > 1
            and local_width % (n * LANES) == 0
            and local_width // n == rows
            and tiles % BLOCK == 0
            and tiles // BLOCK <= MASK_ROWS
        )
        if fits:
            return exchanged_body(n, sides, latents, tile_keys, *rest)
        return gathered_body(latents, tile_keys, *rest)

    return jax.shard_map(
        body,
        mesh=mesh,
        in_specs=placed,
        out_specs=(
            P(("groups", "slide"), "seq", "head"),
            P(("groups", "seq"), "head"),
            P(("groups", "slide"), "seq", "head"),
            P(("groups", "slide"), "seq", "head"),
        ),
        check_vma=False,
    )
```

```python
import functools
import math

import jax
import jax.numpy as jnp
from jax import lax
from jax.experimental import pallas as pl
from jax.experimental.pallas import tpu as pltpu
from jax.sharding import PartitionSpec as P


HD = 64
BLOCK = 128
LANES = 128
MASK_ROWS = 16

masked_score = -1e30


bf16 = jnp.bfloat16
f32 = jnp.float32


def gathered_body(latents, tile_keys, tile_values, tile_mask, latent_counts, out_weight, cotangent):
    local_rows = latents.shape[0]
    local_width = latents.shape[1]
    head_count = local_width // HD
    factor = HD ** (-0.5)
    queries = lax.all_gather(latents, "seq", axis=0, tiled=True)
    total_rows = queries.shape[0]
    first_row = lax.axis_index("seq") * local_rows
    every_row = lax.broadcasted_iota(jnp.int32, (total_rows, 1), 0)
    own_row = lax.broadcasted_iota(jnp.int32, (local_rows, 1), 0) + first_row
    tile_count = tile_keys.shape[1]
    key_block = tile_keys[0]
    value_block = tile_values[0]
    valid_tiles = jnp.broadcast_to(tile_mask[0][:, None] > 0, (tile_count // BLOCK, BLOCK)).reshape(
        1, tile_count
    )
    live_count = latent_counts[0]
    score_list = []
    for which_head in range(head_count):
        columns = slice(which_head * HD, (which_head + 1) * HD)
        raw_scores = (
            jnp.einsum(
                "qc,tc->qt",
                queries[:, columns],
                key_block[:, columns],
                preferred_element_type=jnp.float32,
            )
            * factor
        )
        score_list.append(jnp.where(valid_tiles, raw_scores, masked_score))
    local_top = jnp.stack([jnp.max(scored, axis=1) for scored in score_list], axis=1)
    row_top = lax.pmax(local_top, "seq")
    expo_list = []
    weighted_list = []
    total_list = []
    for which_head in range(head_count):
        columns = slice(which_head * HD, (which_head + 1) * HD)
        expos = jnp.where(
            valid_tiles,
            jnp.exp(score_list[which_head] - row_top[:, which_head : which_head + 1]),
            0.0,
        )
        expo_list.append(expos)
        total_list.append(jnp.sum(expos, axis=1))
        weighted_list.append(
            jnp.dot(
                expos.astype(jnp.bfloat16),
                value_block[:, columns],
                preferred_element_type=jnp.float32,
            )
        )
    partial_sums = jnp.concatenate(weighted_list, axis=1)
    partial_totals = jnp.stack(total_list, axis=1)
    weighted, totals = lax.psum((partial_sums, partial_totals), "seq")
    span = weighted.shape[0]
    attended = jnp.where(
        every_row < live_count,
        (weighted.reshape(span, head_count, HD) / totals[:, :, None]).reshape(span, local_width),
        0.0,
    ).astype(jnp.bfloat16)
    own_attended = lax.dynamic_slice_in_dim(attended, first_row, local_rows, 0)
    pooled_part = jnp.dot(own_attended, out_weight, preferred_element_type=jnp.float32)
    pooled_parts = [
        lax.psum_scatter(pooled_part.astype(jnp.bfloat16), "head", scatter_dimension=1, tiled=True)
    ]
    projected = jnp.einsum(
        "rd,cd->rc", cotangent[0], out_weight, preferred_element_type=jnp.float32
    )
    upstream = jnp.where(own_row < live_count, projected, 0.0).astype(jnp.bfloat16)
    upstream_all = lax.all_gather(upstream, "seq", axis=0, tiled=True)
    row_delta = jnp.sum(
        (upstream_all.astype(jnp.float32) * attended.astype(jnp.float32)).reshape(
            total_rows, head_count, HD
        ),
        axis=2,
    )
    query_list = []
    key_list = []
    value_list = []
    for which_head in range(head_count):
        columns = slice(which_head * HD, (which_head + 1) * HD)
        up_head = upstream_all[:, columns]
        weights = expo_list[which_head] / totals[:, which_head : which_head + 1]
        value_list.append(
            jnp.einsum(
                "qt,qc->tc",
                weights.astype(jnp.bfloat16),
                up_head,
                preferred_element_type=jnp.float32,
            )
        )
        grad_prob = jnp.einsum(
            "qc,tc->qt", up_head, value_block[:, columns], preferred_element_type=jnp.float32
        )
        grad_score = (
            weights * (grad_prob - row_delta[:, which_head : which_head + 1]) * factor
        ).astype(jnp.bfloat16)
        query_list.append(
            jnp.dot(grad_score, key_block[:, columns], preferred_element_type=jnp.float32)
        )
        key_list.append(
            jnp.einsum(
                "qt,qc->tc", grad_score, queries[:, columns], preferred_element_type=jnp.float32
            )
        )
    grad_rows = jnp.concatenate(query_list, axis=1)
    key_grads = [jnp.concatenate(key_list, axis=1).astype(jnp.bfloat16)]
    value_grads = [jnp.concatenate(value_list, axis=1).astype(jnp.bfloat16)]
    own_grad = lax.psum_scatter(
        grad_rows.astype(jnp.bfloat16), "seq", scatter_dimension=0, tiled=True
    )
    grad_latents = lax.psum(own_grad, "slide").astype(jnp.float32)
    return (
        jnp.stack(pooled_parts, axis=0),
        grad_latents,
        jnp.stack(key_grads, axis=0),
        jnp.stack(value_grads, axis=0),
    )


def dot_nn(a, b):
    return lax.dot_general(a, b, (((1,), (0,)), ((), ())), preferred_element_type=f32)


def dot_nt(a, b):
    return lax.dot_general(a, b, (((1,), (1,)), ((), ())), preferred_element_type=f32)


def lane_block(index, width):
    return pl.ds(pl.multiple_of(index * width, width), width)


def pack_kernel(n, mask_ref, keys_ref, latents_ref, values_ref, weight_ref, cot_ref, *rest):
    a_outs, v_outs = rest[:n], rest[n : 2 * n]
    mask, weight, cot, up_ref, sems = rest[2 * n :]
    me = lax.axis_index("seq")
    tiles, width = v_outs[0].shape
    rows = cot.shape[0]
    sources = [
        (mask_ref, mask),
        (weight_ref, weight),
        (cot_ref.at[0], cot),
    ]
    for d in range(n):
        columns = lane_block((me ^ d), width)
        sources.append((keys_ref.at[0, :, columns], a_outs[d].at[:tiles, :]))
        sources.append((latents_ref.at[:, columns], a_outs[d].at[tiles : tiles + rows, :]))
        sources.append((values_ref.at[0, :, columns], v_outs[d]))
    copies = [
        pltpu.make_async_copy(source, target, sems.at[i])
        for i, (source, target) in enumerate(sources)
    ]
    for copy in copies:
        copy.start()
    for copy in copies[:3]:
        copy.wait()
    row_id = lax.broadcasted_iota(jnp.int32, (MASK_ROWS, width), 0)
    flags = jnp.zeros((MASK_ROWS, width), f32)
    for block in range(tiles // BLOCK):
        value = jnp.where(mask[0, block] > 0, 1.0, 0.0)
        flags = jnp.where(row_id == block, value, flags)
    up_ref[...] = dot_nt(weight[...], cot[...]).astype(bf16)
    for d in range(n):
        owner = (me ^ d)
        a_outs[d][tiles + rows : tiles + rows + width, :] = up_ref[lane_block(owner, width), :]
        a_outs[d][tiles + rows + width :, :] = flags.astype(bf16)
    for copy in copies[3:]:
        copy.wait()


def head_mask(h, shape, axis):
    return lax.broadcasted_iota(jnp.int32, shape, axis) // HD == h


def softmax_kernel(n, heads, rows, *refs):
    a_refs = refs[:n]
    expo_ref, total_ref, keys_t_ref, score_ref = refs[n:]
    width = heads * HD
    tiles = expo_ref.shape[2]
    total_rows = n * rows
    per_block = tiles // BLOCK
    scale = HD ** (-0.5) * math.log2(math.e)
    queries = jnp.concatenate([a_refs[d][tiles : tiles + rows, :] for d in range(n)], axis=0)
    queries_t = queries.astype(f32).T.astype(bf16)
    valid = []
    for d in range(n):
        flags = a_refs[d][tiles + rows + width :, :].astype(f32)
        for j in range(per_block):
            valid.append(
                jnp.concatenate([flags[j : j + 1, :]] * (total_rows // width), axis=1) > 0.5
            )
    for h in range(heads):
        top = jnp.full((1, total_rows), masked_score, f32)
        query_h = jnp.where(
            head_mask(h, (width, total_rows), 0), queries_t, jnp.zeros_like(queries_t)
        )
        for d in range(n):
            scored = dot_nn(a_refs[d][:tiles, :], query_h)
            score_ref[d] = scored
            for j in range(per_block):
                block_top = jnp.max(scored[j * BLOCK : (j + 1) * BLOCK], axis=0, keepdims=True)
                top = jnp.maximum(top, jnp.where(valid[d * per_block + j], block_top, masked_score))
        total = jnp.zeros((1, total_rows), f32)
        for d in range(n):
            for j in range(per_block):
                part = slice(j * BLOCK, (j + 1) * BLOCK)
                expos = jnp.where(
                    valid[d * per_block + j], jnp.exp2((score_ref[d, part, :] - top) * scale), 0.0
                )
                total = total + jnp.sum(expos, axis=0, keepdims=True)
                expo_ref[h, d, part, :] = expos.astype(bf16)
        total_ref[h] = total
    for d in range(n):
        keys_t_ref[d] = a_refs[d][:tiles, :].astype(f32).T.astype(bf16)


def live_kernel(n, count_ref, live_ref):
    me = lax.axis_index("seq")
    rows = live_ref.shape[1] // n
    lane_row = lax.broadcasted_iota(jnp.int32, (1, rows), 1)
    for d in range(n):
        source_row = lane_row + (me ^ d) * rows
        live_ref[:, d * rows : (d + 1) * rows] = jnp.where(source_row < count_ref[0], 1.0, 0.0)


def value_grads_kernel(n, heads, live_ref, expo_ref, total_ref, *refs):
    a_refs, up_ref, outs = refs[:n], refs[n], refs[n + 1 :]
    factor = HD ** (-0.5)
    width = heads * HD
    first = a_refs[0].shape[0] - MASK_ROWS - width
    upstream_t = jnp.concatenate(
        [a_refs[d][first : first + width, :] for d in range(n)], axis=1
    )
    live = live_ref[...] > 0.5
    up_scaled_t = jnp.concatenate(
        [
            jnp.where(
                live, upstream_t[h * HD : (h + 1) * HD, :].astype(f32) * (factor / total_ref[h]), 0.0
            )
            for h in range(heads)
        ],
        axis=0,
    )
    up_ref[...] = up_scaled_t.astype(bf16)
    up_scaled = up_scaled_t.T
    up_heads = [
        jnp.where(head_mask(h, up_scaled.shape, 1), up_scaled, 0.0).astype(bf16)
        for h in range(heads)
    ]
    for d in range(n):
        value_grad = dot_nn(expo_ref[0, d], up_heads[0])
        for h in range(1, heads):
            value_grad = value_grad + dot_nn(expo_ref[h, d], up_heads[h])
        outs[d][...] = (value_grad * (1.0 / factor)).astype(bf16)


def key_grads_kernel(n, heads, rows, live_ref, expo_ref, total_ref, up_ref, keys_t_ref, *refs):
    a_refs, v_refs = refs[:n], refs[n : 2 * n]
    outs, query_grad_ref = refs[2 * n : 3 * n], refs[3 * n]
    width = heads * HD
    tiles = v_refs[0].shape[0]
    total_rows = n * rows
    live = live_ref[...] > 0.5
    queries = jnp.concatenate([a_refs[d][tiles : tiles + rows, :] for d in range(n)], axis=0)
    up_scaled_t = up_ref[...]
    values_t = [v_refs[d][...].astype(f32).T.astype(bf16) for d in range(n)]
    attended_list = []
    delta_list = []
    for h in range(heads):
        own_rows = slice(h * HD, (h + 1) * HD)
        weighted = dot_nn(values_t[0][own_rows, :], expo_ref[h, 0])
        for d in range(1, n):
            weighted = weighted + dot_nn(values_t[d][own_rows, :], expo_ref[h, d])
        attended_h = jnp.where(live, weighted / total_ref[h], 0.0).astype(bf16)
        delta_list.append(
            jnp.sum(
                up_scaled_t[own_rows, :].astype(f32) * attended_h.astype(f32),
                axis=0,
                keepdims=True,
            )
        )
        attended_list.append(attended_h)
    attended = jnp.concatenate(attended_list, axis=0)
    zero_rows = jnp.zeros_like(queries)
    zero_cols = jnp.zeros_like(up_scaled_t)
    query_heads = [jnp.where(head_mask(h, queries.shape, 1), queries, zero_rows) for h in range(heads)]
    up_heads_t = [
        jnp.where(head_mask(h, up_scaled_t.shape, 0), up_scaled_t, zero_cols) for h in range(heads)
    ]
    query_grad = [jnp.zeros((HD, total_rows), f32) for _ in range(heads)]
    for d in range(n):
        key_grad = jnp.zeros((tiles, width), f32)
        for h in range(heads):
            grad_prob = dot_nn(v_refs[d][...], up_heads_t[h])
            grad_score = (expo_ref[h, d].astype(f32) * (grad_prob - delta_list[h])).astype(bf16)
            key_grad = key_grad + dot_nn(grad_score, query_heads[h])
            query_grad[h] = query_grad[h] + dot_nn(
                keys_t_ref[d, h * HD : (h + 1) * HD, :], grad_score
            )
        outs[d][:tiles, :] = key_grad.astype(bf16)
        outs[d][tiles:, :] = attended[:, d * rows : (d + 1) * rows]
    query_grad_ref[...] = jnp.concatenate(query_grad, axis=0).astype(bf16)


def values_home_kernel(n, *refs):
    c_refs, value_grad_ref = refs[:n], refs[n]
    me = lax.axis_index("seq")
    width = c_refs[0].shape[1]
    for d in range(n):
        value_grad_ref[0, :, lane_block((me ^ d), width)] = c_refs[d][...]


def pool_kernel(n, weight_ref, *refs):
    k_refs = refs[:n]
    key_grad_ref, kept_ref, sent_ref = refs[n : n + 3]
    me, side = lax.axis_index("seq"), lax.axis_index("head")
    width = k_refs[0].shape[1]
    tiles = key_grad_ref.shape[1]
    half = kept_ref.shape[1]
    kept = jnp.zeros(kept_ref.shape, f32)
    sent = jnp.zeros(sent_ref.shape, f32)
    for d in range(n):
        owner = (me ^ d)
        key_grad_ref[0, :, lane_block(owner, width)] = k_refs[d][:tiles, :]
        attended = k_refs[d][tiles:, :].astype(f32).T.astype(bf16)
        inputs = lane_block(owner, width)
        kept = kept + dot_nn(attended, weight_ref[inputs, lane_block(side, half)])
        sent = sent + dot_nn(attended, weight_ref[inputs, lane_block(1 - side, half)])
    kept_ref[...] = kept
    sent_ref[...] = sent.astype(bf16)


def join_kernel(n, own_ref, other_ref, *outs):
    rows = outs[0].shape[1]
    both = (own_ref[...].astype(f32) + other_ref[...].astype(f32)).astype(bf16)
    for d in range(n):
        outs[d][...] = both[:, d * rows : (d + 1) * rows]


def last_kernel(n, kept_ref, came_ref, *refs):
    g_refs, latent_grad_ref, pooled_ref = refs[:n], refs[n], refs[n + 1]
    me = lax.axis_index("seq")
    width = g_refs[0].shape[0]
    for d in range(n):
        columns = lane_block((me ^ d), width)
        latent_grad_ref[:, columns] = g_refs[d][...].astype(f32).T
    pooled_ref[0] = (kept_ref[...] + came_ref[...].astype(f32)).astype(bf16)


SMEM = pl.BlockSpec(memory_space=pltpu.SMEM)
HBM = pl.BlockSpec(memory_space=pltpu.HBM)
VMEM = pl.BlockSpec(memory_space=pltpu.VMEM)


def call(kernel, out_shape, operands, flops, scratch=(), grant=8, spaces=None):
    moved = sum(x.size * x.dtype.itemsize for x in operands)
    moved += sum(math.prod(x.shape) * x.dtype.itemsize for x in out_shape)
    return pl.pallas_call(
        kernel,
        out_shape=out_shape,
        in_specs=spaces or [VMEM] * len(operands),
        out_specs=[VMEM] * len(out_shape),
        scratch_shapes=list(scratch),
        cost_estimate=pl.CostEstimate(flops=int(flops), bytes_accessed=moved, transcendentals=0),
        compiler_params=pltpu.CompilerParams(vmem_limit_bytes=grant * 1024 * 1024),
    )(*operands)


def exchanged_body(n, sides, latents, tile_keys, tile_values, tile_mask, latent_counts, out_weight, cotangent):
    rows, local_width = latents.shape
    tiles = tile_keys.shape[1]
    out_width = out_weight.shape[1]
    heads = local_width // HD // n
    width = heads * HD
    total_rows = n * rows
    sds = jax.ShapeDtypeStruct
    product = 2 * total_rows * n * tiles * width

    def spread(pieces):
        came = {0: pieces[0]}
        for d in offsets(n):
            came[d] = lax.ppermute(pieces[d], "seq", [(i, i ^ d) for i in range(n)])
        return [came[d] for d in range(n)]

    packed = call(
        functools.partial(pack_kernel, n),
        [sds((tiles + rows + width + MASK_ROWS, width), bf16)] * n
        + [sds((tiles, width), bf16)] * n,
        tuple(
            pltpu.with_memory_space_constraint(x, pltpu.HBM)
            for x in (tile_mask, tile_keys, latents, tile_values, out_weight, cotangent)
        ),
        2 * rows * local_width * out_width,
        [
            pltpu.SMEM(tile_mask.shape, jnp.int32),
            pltpu.VMEM(out_weight.shape, bf16),
            pltpu.VMEM(cotangent.shape[1:], bf16),
            pltpu.VMEM((local_width, rows), bf16),
            pltpu.SemaphoreType.DMA((3 + 3 * n,)),
        ],
        spaces=[HBM] * 6,
    )
    a_list = spread(packed[:n])
    v_list = spread(packed[n:])
    expos, totals, keys_t = call(
        functools.partial(softmax_kernel, n, heads, rows),
        [
            sds((heads, n, tiles, total_rows), bf16),
            sds((heads, 1, total_rows), f32),
            sds((n, width, tiles), bf16),
        ],
        a_list,
        product,
        [pltpu.VMEM((n, tiles, total_rows), f32)],
        16,
    )
    (live,) = call(
        functools.partial(live_kernel, n),
        [sds((1, total_rows), f32)],
        (latent_counts,),
        1e4,
        spaces=[SMEM],
    )
    up_scaled, *c_out = call(
        functools.partial(value_grads_kernel, n, heads),
        [sds((width, total_rows), bf16)] + [sds((tiles, width), bf16)] * n,
        (live, expos, totals, *a_list),
        product,
        (),
        16,
    )
    c_list = spread(c_out)
    *k_out, query_grad = call(
        functools.partial(key_grads_kernel, n, heads, rows),
        [sds((tiles + width, width), bf16)] * n + [sds((width, total_rows), bf16)],
        (live, expos, totals, up_scaled, keys_t, *a_list, *v_list),
        4 * product,
        (),
        16,
    )
    other_sum = None
    for step in range(1, sides):
        came = lax.ppermute(query_grad, "slide", [(i, (i + step) % sides) for i in range(sides)])
        other_sum = came if other_sum is None else other_sum.astype(f32) + came.astype(f32)
    k_list = spread(k_out)
    joined = call(
        functools.partial(join_kernel, n),
        [sds((width, rows), bf16)] * n,
        (query_grad, other_sum),
        1e6,
    )
    g_list = spread(joined)
    (value_grads,) = call(
        functools.partial(values_home_kernel, n), [sds(tile_values.shape, bf16)], c_list, 1e6
    )
    key_grads, kept, sent = call(
        functools.partial(pool_kernel, n),
        [
            sds(tile_keys.shape, bf16),
            sds((rows, out_width // 2), f32),
            sds((rows, out_width // 2), bf16),
        ],
        (out_weight, *k_list),
        2 * rows * local_width * out_width,
    )
    came = lax.ppermute(sent, "head", [(0, 1), (1, 0)])
    latent_grads, pooled = call(
        functools.partial(last_kernel, n),
        [sds(latents.shape, f32), sds((1, rows, out_width // 2), bf16)],
        (kept, came, *g_list),
        1e6,
    )
    return pooled, latent_grads, key_grads, value_grads


def offsets(n):
    return [*range(n // 2, n), *range(n // 2 - 1, 0, -1)]


def solution(mesh):
    placed = (
        P(("groups", "seq"), "head"),
        P(("groups", "slide"), "seq", "head"),
        P(("groups", "slide"), "seq", "head"),
        P(("groups", "slide"), "seq"),
        P(("groups", "slide")),
        P("head", None),
        P(("groups", "slide"), "seq", None),
    )
    n, sides = mesh.shape["seq"], mesh.shape["slide"]

    def body(latents, tile_keys, *rest):
        rows, local_width = latents.shape
        tiles = tile_keys.shape[1]
        fits = (
            mesh.shape["head"] == 2
            and sides > 1
            and local_width % (n * LANES) == 0
            and local_width // n == rows
            and tiles % BLOCK == 0
            and tiles // BLOCK <= MASK_ROWS
            and n >= 4
            and n & (n - 1) == 0
        )
        if fits:
            return exchanged_body(n, sides, latents, tile_keys, *rest)
        return gathered_body(latents, tile_keys, *rest)

    return jax.shard_map(
        body,
        mesh=mesh,
        in_specs=placed,
        out_specs=(
            P(("groups", "slide"), "seq", "head"),
            P(("groups", "seq"), "head"),
            P(("groups", "slide"), "seq", "head"),
            P(("groups", "slide"), "seq", "head"),
        ),
        check_vma=False,
    )
```

```python
import functools
import math

import jax
import jax.numpy as jnp
from jax import lax
from jax.experimental import pallas as pl
from jax.experimental.pallas import tpu as pltpu
from jax.sharding import PartitionSpec as P


HD = 64
BLOCK = 128
LANES = 128
MASK_ROWS = 16

masked_score = -1e30


bf16 = jnp.bfloat16
f32 = jnp.float32


def gathered_body(latents, tile_keys, tile_values, tile_mask, latent_counts, out_weight, cotangent):
    local_rows = latents.shape[0]
    local_width = latents.shape[1]
    head_count = local_width // HD
    factor = HD ** (-0.5)
    queries = lax.all_gather(latents, "seq", axis=0, tiled=True)
    total_rows = queries.shape[0]
    first_row = lax.axis_index("seq") * local_rows
    every_row = lax.broadcasted_iota(jnp.int32, (total_rows, 1), 0)
    own_row = lax.broadcasted_iota(jnp.int32, (local_rows, 1), 0) + first_row
    tile_count = tile_keys.shape[1]
    key_block = tile_keys[0]
    value_block = tile_values[0]
    valid_tiles = jnp.broadcast_to(tile_mask[0][:, None] > 0, (tile_count // BLOCK, BLOCK)).reshape(
        1, tile_count
    )
    live_count = latent_counts[0]
    score_list = []
    for which_head in range(head_count):
        columns = slice(which_head * HD, (which_head + 1) * HD)
        raw_scores = (
            jnp.einsum(
                "qc,tc->qt",
                queries[:, columns],
                key_block[:, columns],
                preferred_element_type=jnp.float32,
            )
            * factor
        )
        score_list.append(jnp.where(valid_tiles, raw_scores, masked_score))
    local_top = jnp.stack([jnp.max(scored, axis=1) for scored in score_list], axis=1)
    row_top = lax.pmax(local_top, "seq")
    expo_list = []
    weighted_list = []
    total_list = []
    for which_head in range(head_count):
        columns = slice(which_head * HD, (which_head + 1) * HD)
        expos = jnp.where(
            valid_tiles,
            jnp.exp(score_list[which_head] - row_top[:, which_head : which_head + 1]),
            0.0,
        )
        expo_list.append(expos)
        total_list.append(jnp.sum(expos, axis=1))
        weighted_list.append(
            jnp.dot(
                expos.astype(jnp.bfloat16),
                value_block[:, columns],
                preferred_element_type=jnp.float32,
            )
        )
    partial_sums = jnp.concatenate(weighted_list, axis=1)
    partial_totals = jnp.stack(total_list, axis=1)
    weighted, totals = lax.psum((partial_sums, partial_totals), "seq")
    span = weighted.shape[0]
    attended = jnp.where(
        every_row < live_count,
        (weighted.reshape(span, head_count, HD) / totals[:, :, None]).reshape(span, local_width),
        0.0,
    ).astype(jnp.bfloat16)
    own_attended = lax.dynamic_slice_in_dim(attended, first_row, local_rows, 0)
    pooled_part = jnp.dot(own_attended, out_weight, preferred_element_type=jnp.float32)
    pooled_parts = [
        lax.psum_scatter(pooled_part.astype(jnp.bfloat16), "head", scatter_dimension=1, tiled=True)
    ]
    projected = jnp.einsum(
        "rd,cd->rc", cotangent[0], out_weight, preferred_element_type=jnp.float32
    )
    upstream = jnp.where(own_row < live_count, projected, 0.0).astype(jnp.bfloat16)
    upstream_all = lax.all_gather(upstream, "seq", axis=0, tiled=True)
    row_delta = jnp.sum(
        (upstream_all.astype(jnp.float32) * attended.astype(jnp.float32)).reshape(
            total_rows, head_count, HD
        ),
        axis=2,
    )
    query_list = []
    key_list = []
    value_list = []
    for which_head in range(head_count):
        columns = slice(which_head * HD, (which_head + 1) * HD)
        up_head = upstream_all[:, columns]
        weights = expo_list[which_head] / totals[:, which_head : which_head + 1]
        value_list.append(
            jnp.einsum(
                "qt,qc->tc",
                weights.astype(jnp.bfloat16),
                up_head,
                preferred_element_type=jnp.float32,
            )
        )
        grad_prob = jnp.einsum(
            "qc,tc->qt", up_head, value_block[:, columns], preferred_element_type=jnp.float32
        )
        grad_score = (
            weights * (grad_prob - row_delta[:, which_head : which_head + 1]) * factor
        ).astype(jnp.bfloat16)
        query_list.append(
            jnp.dot(grad_score, key_block[:, columns], preferred_element_type=jnp.float32)
        )
        key_list.append(
            jnp.einsum(
                "qt,qc->tc", grad_score, queries[:, columns], preferred_element_type=jnp.float32
            )
        )
    grad_rows = jnp.concatenate(query_list, axis=1)
    key_grads = [jnp.concatenate(key_list, axis=1).astype(jnp.bfloat16)]
    value_grads = [jnp.concatenate(value_list, axis=1).astype(jnp.bfloat16)]
    own_grad = lax.psum_scatter(
        grad_rows.astype(jnp.bfloat16), "seq", scatter_dimension=0, tiled=True
    )
    grad_latents = lax.psum(own_grad, "slide").astype(jnp.float32)
    return (
        jnp.stack(pooled_parts, axis=0),
        grad_latents,
        jnp.stack(key_grads, axis=0),
        jnp.stack(value_grads, axis=0),
    )


def dot_nn(a, b):
    return lax.dot_general(a, b, (((1,), (0,)), ((), ())), preferred_element_type=f32)


def dot_nt(a, b):
    return lax.dot_general(a, b, (((1,), (1,)), ((), ())), preferred_element_type=f32)


def lane_block(index, width):
    return pl.ds(pl.multiple_of(index * width, width), width)


def pack_keys_kernel(n, mask_ref, keys_ref, latents_ref, *rest):
    outs, mask, sems = rest[:n], rest[n], rest[n + 1]
    me = lax.axis_index("seq")
    tiles, rows, width = keys_ref.shape[1], latents_ref.shape[0], outs[0].shape[1]
    sources = [(mask_ref, mask)]
    for d in range(n):
        columns = lane_block(me ^ d, width)
        sources.append((keys_ref.at[0, :, columns], outs[d].at[:tiles, :]))
        sources.append((latents_ref.at[:, columns], outs[d].at[tiles : tiles + rows, :]))
    copies = [
        pltpu.make_async_copy(source, target, sems.at[i])
        for i, (source, target) in enumerate(sources)
    ]
    for copy in copies:
        copy.start()
    copies[0].wait()
    row_id = lax.broadcasted_iota(jnp.int32, (MASK_ROWS, width), 0)
    flags = jnp.zeros((MASK_ROWS, width), f32)
    for block in range(tiles // BLOCK):
        value = jnp.where(mask[0, block] > 0, 1.0, 0.0)
        flags = jnp.where(row_id == block, value, flags)
    for d in range(n):
        outs[d][tiles + rows :, :] = flags.astype(bf16)
    for copy in copies[1:]:
        copy.wait()


def pack_values_kernel(n, count_ref, values_ref, weight_ref, cot_ref, *rest):
    u_outs, v_outs, live_ref = rest[:n], rest[n : 2 * n], rest[2 * n]
    weight, cot, up_ref, sems = rest[2 * n + 1 :]
    me = lax.axis_index("seq")
    width, rows = u_outs[0].shape
    sources = [(weight_ref, weight), (cot_ref.at[0], cot)]
    for d in range(n):
        sources.append((values_ref.at[0, :, lane_block(me ^ d, width)], v_outs[d]))
    copies = [
        pltpu.make_async_copy(source, target, sems.at[i])
        for i, (source, target) in enumerate(sources)
    ]
    for copy in copies:
        copy.start()
    lane_row = lax.broadcasted_iota(jnp.int32, (1, rows), 1)
    for d in range(n):
        source_row = lane_row + (me ^ d) * rows
        live_ref[:, d * rows : (d + 1) * rows] = jnp.where(source_row < count_ref[0], 1.0, 0.0)
    for copy in copies[:2]:
        copy.wait()
    up_ref[...] = dot_nt(weight[...], cot[...]).astype(bf16)
    for d in range(n):
        u_outs[d][...] = up_ref[lane_block(me ^ d, width), :]
    for copy in copies[2:]:
        copy.wait()


def head_mask(h, shape, axis):
    return lax.broadcasted_iota(jnp.int32, shape, axis) // HD == h


def softmax_kernel(n, heads, rows, *refs):
    a_refs = refs[:n]
    expo_ref, total_ref, keys_t_ref, score_ref = refs[n:]
    width = heads * HD
    tiles = expo_ref.shape[2]
    total_rows = n * rows
    per_block = tiles // BLOCK
    scale = HD ** (-0.5) * math.log2(math.e)
    queries = jnp.concatenate([a_refs[d][tiles : tiles + rows, :] for d in range(n)], axis=0)
    queries_t = queries.astype(f32).T.astype(bf16)
    valid = []
    for d in range(n):
        flags = a_refs[d][tiles + rows :, :].astype(f32)
        for j in range(per_block):
            valid.append(
                jnp.concatenate([flags[j : j + 1, :]] * (total_rows // width), axis=1) > 0.5
            )
    for h in range(heads):
        top = jnp.full((1, total_rows), masked_score, f32)
        query_h = jnp.where(
            head_mask(h, (width, total_rows), 0), queries_t, jnp.zeros_like(queries_t)
        )
        for d in range(n):
            scored = dot_nn(a_refs[d][:tiles, :], query_h)
            score_ref[d] = scored
            for j in range(per_block):
                block_top = jnp.max(scored[j * BLOCK : (j + 1) * BLOCK], axis=0, keepdims=True)
                top = jnp.maximum(top, jnp.where(valid[d * per_block + j], block_top, masked_score))
        total = jnp.zeros((1, total_rows), f32)
        for d in range(n):
            for j in range(per_block):
                part = slice(j * BLOCK, (j + 1) * BLOCK)
                expos = jnp.where(
                    valid[d * per_block + j], jnp.exp2((score_ref[d, part, :] - top) * scale), 0.0
                )
                total = total + jnp.sum(expos, axis=0, keepdims=True)
                expo_ref[h, d, part, :] = expos.astype(bf16)
        total_ref[h] = total
    for d in range(n):
        keys_t_ref[d] = a_refs[d][:tiles, :].astype(f32).T.astype(bf16)


def value_grads_kernel(n, heads, live_ref, expo_ref, total_ref, *refs):
    u_refs, up_ref, outs = refs[:n], refs[n], refs[n + 1 :]
    factor = HD ** (-0.5)
    upstream_t = jnp.concatenate([u_refs[d][...] for d in range(n)], axis=1)
    live = live_ref[...] > 0.5
    up_scaled_t = jnp.concatenate(
        [
            jnp.where(
                live, upstream_t[h * HD : (h + 1) * HD, :].astype(f32) * (factor / total_ref[h]), 0.0
            )
            for h in range(heads)
        ],
        axis=0,
    )
    up_ref[...] = up_scaled_t.astype(bf16)
    up_scaled = up_scaled_t.T
    up_heads = [
        jnp.where(head_mask(h, up_scaled.shape, 1), up_scaled, 0.0).astype(bf16)
        for h in range(heads)
    ]
    for d in range(n):
        value_grad = dot_nn(expo_ref[0, d], up_heads[0])
        for h in range(1, heads):
            value_grad = value_grad + dot_nn(expo_ref[h, d], up_heads[h])
        outs[d][...] = (value_grad * (1.0 / factor)).astype(bf16)


def key_grads_kernel(n, heads, rows, live_ref, expo_ref, total_ref, up_ref, keys_t_ref, *refs):
    a_refs, v_refs = refs[:n], refs[n : 2 * n]
    outs, query_grad_ref = refs[2 * n : 3 * n], refs[3 * n]
    width = heads * HD
    tiles = v_refs[0].shape[0]
    total_rows = n * rows
    live = live_ref[...] > 0.5
    queries = jnp.concatenate([a_refs[d][tiles : tiles + rows, :] for d in range(n)], axis=0)
    up_scaled_t = up_ref[...]
    values_t = [v_refs[d][...].astype(f32).T.astype(bf16) for d in range(n)]
    attended_list = []
    delta_list = []
    for h in range(heads):
        own_rows = slice(h * HD, (h + 1) * HD)
        weighted = dot_nn(values_t[0][own_rows, :], expo_ref[h, 0])
        for d in range(1, n):
            weighted = weighted + dot_nn(values_t[d][own_rows, :], expo_ref[h, d])
        attended_h = jnp.where(live, weighted / total_ref[h], 0.0).astype(bf16)
        delta_list.append(
            jnp.sum(
                up_scaled_t[own_rows, :].astype(f32) * attended_h.astype(f32),
                axis=0,
                keepdims=True,
            )
        )
        attended_list.append(attended_h)
    attended = jnp.concatenate(attended_list, axis=0)
    zero_rows = jnp.zeros_like(queries)
    zero_cols = jnp.zeros_like(up_scaled_t)
    query_heads = [jnp.where(head_mask(h, queries.shape, 1), queries, zero_rows) for h in range(heads)]
    up_heads_t = [
        jnp.where(head_mask(h, up_scaled_t.shape, 0), up_scaled_t, zero_cols) for h in range(heads)
    ]
    query_grad = [jnp.zeros((HD, total_rows), f32) for _ in range(heads)]
    for d in range(n):
        key_grad = jnp.zeros((tiles, width), f32)
        for h in range(heads):
            grad_prob = dot_nn(v_refs[d][...], up_heads_t[h])
            grad_score = (expo_ref[h, d].astype(f32) * (grad_prob - delta_list[h])).astype(bf16)
            key_grad = key_grad + dot_nn(grad_score, query_heads[h])
            query_grad[h] = query_grad[h] + dot_nn(
                keys_t_ref[d, h * HD : (h + 1) * HD, :], grad_score
            )
        outs[d][:tiles, :] = key_grad.astype(bf16)
        outs[d][tiles:, :] = attended[:, d * rows : (d + 1) * rows]
    query_grad_ref[...] = jnp.concatenate(query_grad, axis=0).astype(bf16)


def values_home_kernel(n, *refs):
    c_refs, value_grad_ref = refs[:n], refs[n]
    me = lax.axis_index("seq")
    width = c_refs[0].shape[1]
    for d in range(n):
        value_grad_ref[0, :, lane_block((me ^ d), width)] = c_refs[d][...]


def pool_kernel(n, weight_ref, *refs):
    k_refs = refs[:n]
    key_grad_ref, kept_ref, sent_ref = refs[n : n + 3]
    me, side = lax.axis_index("seq"), lax.axis_index("head")
    width = k_refs[0].shape[1]
    tiles = key_grad_ref.shape[1]
    half = kept_ref.shape[1]
    kept = jnp.zeros(kept_ref.shape, f32)
    sent = jnp.zeros(sent_ref.shape, f32)
    for d in range(n):
        owner = (me ^ d)
        key_grad_ref[0, :, lane_block(owner, width)] = k_refs[d][:tiles, :]
        attended = k_refs[d][tiles:, :].astype(f32).T.astype(bf16)
        inputs = lane_block(owner, width)
        kept = kept + dot_nn(attended, weight_ref[inputs, lane_block(side, half)])
        sent = sent + dot_nn(attended, weight_ref[inputs, lane_block(1 - side, half)])
    kept_ref[...] = kept
    sent_ref[...] = sent.astype(bf16)


def join_kernel(n, own_ref, other_ref, *outs):
    rows = outs[0].shape[1]
    both = (own_ref[...].astype(f32) + other_ref[...].astype(f32)).astype(bf16)
    for d in range(n):
        outs[d][...] = both[:, d * rows : (d + 1) * rows]


def last_kernel(n, kept_ref, came_ref, *refs):
    g_refs, latent_grad_ref, pooled_ref = refs[:n], refs[n], refs[n + 1]
    me = lax.axis_index("seq")
    width = g_refs[0].shape[0]
    for d in range(n):
        columns = lane_block((me ^ d), width)
        latent_grad_ref[:, columns] = g_refs[d][...].astype(f32).T
    pooled_ref[0] = (kept_ref[...] + came_ref[...].astype(f32)).astype(bf16)


SMEM = pl.BlockSpec(memory_space=pltpu.SMEM)
HBM = pl.BlockSpec(memory_space=pltpu.HBM)
VMEM = pl.BlockSpec(memory_space=pltpu.VMEM)


def call(kernel, out_shape, operands, flops, scratch=(), grant=8, spaces=None):
    moved = sum(x.size * x.dtype.itemsize for x in operands)
    moved += sum(math.prod(x.shape) * x.dtype.itemsize for x in out_shape)
    return pl.pallas_call(
        kernel,
        out_shape=out_shape,
        in_specs=spaces or [VMEM] * len(operands),
        out_specs=[VMEM] * len(out_shape),
        scratch_shapes=list(scratch),
        cost_estimate=pl.CostEstimate(flops=int(flops), bytes_accessed=moved, transcendentals=0),
        compiler_params=pltpu.CompilerParams(vmem_limit_bytes=grant * 1024 * 1024),
    )(*operands)


def exchanged_body(n, sides, latents, tile_keys, tile_values, tile_mask, latent_counts, out_weight, cotangent):
    rows, local_width = latents.shape
    tiles = tile_keys.shape[1]
    out_width = out_weight.shape[1]
    heads = local_width // HD // n
    width = heads * HD
    total_rows = n * rows
    sds = jax.ShapeDtypeStruct
    product = 2 * total_rows * n * tiles * width

    def spread(pieces):
        came = {0: pieces[0]}
        for d in offsets(n):
            came[d] = lax.ppermute(pieces[d], "seq", [(i, i ^ d) for i in range(n)])
        return [came[d] for d in range(n)]

    def in_hbm(*arrays):
        return tuple(pltpu.with_memory_space_constraint(x, pltpu.HBM) for x in arrays)

    packed = call(
        functools.partial(pack_keys_kernel, n),
        [sds((tiles + rows + MASK_ROWS, width), bf16)] * n,
        in_hbm(tile_mask, tile_keys, latents),
        1e6,
        [pltpu.SMEM(tile_mask.shape, jnp.int32), pltpu.SemaphoreType.DMA((1 + 2 * n,))],
        spaces=[HBM] * 3,
    )
    a_list = spread(packed)
    *packed, live = call(
        functools.partial(pack_values_kernel, n),
        [sds((width, rows), bf16)] * n
        + [sds((tiles, width), bf16)] * n
        + [sds((1, total_rows), f32)],
        (latent_counts, *in_hbm(tile_values, out_weight, cotangent)),
        2 * rows * local_width * out_width,
        [
            pltpu.VMEM(out_weight.shape, bf16),
            pltpu.VMEM(cotangent.shape[1:], bf16),
            pltpu.VMEM((local_width, rows), bf16),
            pltpu.SemaphoreType.DMA((2 + n,)),
        ],
        spaces=[SMEM] + [HBM] * 3,
    )
    u_list = spread(packed[:n])
    v_list = spread(packed[n:])
    expos, totals, keys_t = call(
        functools.partial(softmax_kernel, n, heads, rows),
        [
            sds((heads, n, tiles, total_rows), bf16),
            sds((heads, 1, total_rows), f32),
            sds((n, width, tiles), bf16),
        ],
        a_list,
        product,
        [pltpu.VMEM((n, tiles, total_rows), f32)],
        16,
    )
    up_scaled, *c_out = call(
        functools.partial(value_grads_kernel, n, heads),
        [sds((width, total_rows), bf16)] + [sds((tiles, width), bf16)] * n,
        (live, expos, totals, *u_list),
        product,
        (),
        16,
    )
    c_list = spread(c_out)
    *k_out, query_grad = call(
        functools.partial(key_grads_kernel, n, heads, rows),
        [sds((tiles + width, width), bf16)] * n + [sds((width, total_rows), bf16)],
        (live, expos, totals, up_scaled, keys_t, *a_list, *v_list),
        4 * product,
        (),
        16,
    )
    other_sum = None
    for step in range(1, sides):
        came = lax.ppermute(query_grad, "slide", [(i, (i + step) % sides) for i in range(sides)])
        other_sum = came if other_sum is None else other_sum.astype(f32) + came.astype(f32)
    k_list = spread(k_out)
    joined = call(
        functools.partial(join_kernel, n),
        [sds((width, rows), bf16)] * n,
        (query_grad, other_sum),
        1e6,
    )
    g_list = spread(joined)
    (value_grads,) = call(
        functools.partial(values_home_kernel, n), [sds(tile_values.shape, bf16)], c_list, 1e6
    )
    key_grads, kept, sent = call(
        functools.partial(pool_kernel, n),
        [
            sds(tile_keys.shape, bf16),
            sds((rows, out_width // 2), f32),
            sds((rows, out_width // 2), bf16),
        ],
        (out_weight, *k_list),
        2 * rows * local_width * out_width,
    )
    came = lax.ppermute(sent, "head", [(0, 1), (1, 0)])
    latent_grads, pooled = call(
        functools.partial(last_kernel, n),
        [sds(latents.shape, f32), sds((1, rows, out_width // 2), bf16)],
        (kept, came, *g_list),
        1e6,
    )
    return pooled, latent_grads, key_grads, value_grads


def offsets(n):
    return [*range(n // 2, n), *range(n // 2 - 1, 0, -1)]


def solution(mesh):
    placed = (
        P(("groups", "seq"), "head"),
        P(("groups", "slide"), "seq", "head"),
        P(("groups", "slide"), "seq", "head"),
        P(("groups", "slide"), "seq"),
        P(("groups", "slide")),
        P("head", None),
        P(("groups", "slide"), "seq", None),
    )
    n, sides = mesh.shape["seq"], mesh.shape["slide"]

    def body(latents, tile_keys, *rest):
        rows, local_width = latents.shape
        tiles = tile_keys.shape[1]
        fits = (
            mesh.shape["head"] == 2
            and sides > 1
            and local_width % (n * LANES) == 0
            and local_width // n == rows
            and tiles % BLOCK == 0
            and tiles // BLOCK <= MASK_ROWS
            and n >= 4
            and n & (n - 1) == 0
        )
        if fits:
            return exchanged_body(n, sides, latents, tile_keys, *rest)
        return gathered_body(latents, tile_keys, *rest)

    return jax.shard_map(
        body,
        mesh=mesh,
        in_specs=placed,
        out_specs=(
            P(("groups", "slide"), "seq", "head"),
            P(("groups", "seq"), "head"),
            P(("groups", "slide"), "seq", "head"),
            P(("groups", "slide"), "seq", "head"),
        ),
        check_vma=False,
    )
```

```python
import functools
import math

import jax
import jax.numpy as jnp
from jax import lax
from jax.experimental import pallas as pl
from jax.experimental.pallas import tpu as pltpu
from jax.sharding import PartitionSpec as P


HD = 64
BLOCK = 128
LANES = 128
MASK_ROWS = 16

masked_score = -1e30


bf16 = jnp.bfloat16
f32 = jnp.float32


def gathered_body(latents, tile_keys, tile_values, tile_mask, latent_counts, out_weight, cotangent):
    local_rows = latents.shape[0]
    local_width = latents.shape[1]
    head_count = local_width // HD
    factor = HD ** (-0.5)
    queries = lax.all_gather(latents, "seq", axis=0, tiled=True)
    total_rows = queries.shape[0]
    first_row = lax.axis_index("seq") * local_rows
    every_row = lax.broadcasted_iota(jnp.int32, (total_rows, 1), 0)
    own_row = lax.broadcasted_iota(jnp.int32, (local_rows, 1), 0) + first_row
    tile_count = tile_keys.shape[1]
    key_block = tile_keys[0]
    value_block = tile_values[0]
    valid_tiles = jnp.broadcast_to(tile_mask[0][:, None] > 0, (tile_count // BLOCK, BLOCK)).reshape(
        1, tile_count
    )
    live_count = latent_counts[0]
    score_list = []
    for which_head in range(head_count):
        columns = slice(which_head * HD, (which_head + 1) * HD)
        raw_scores = (
            jnp.einsum(
                "qc,tc->qt",
                queries[:, columns],
                key_block[:, columns],
                preferred_element_type=jnp.float32,
            )
            * factor
        )
        score_list.append(jnp.where(valid_tiles, raw_scores, masked_score))
    local_top = jnp.stack([jnp.max(scored, axis=1) for scored in score_list], axis=1)
    row_top = lax.pmax(local_top, "seq")
    expo_list = []
    weighted_list = []
    total_list = []
    for which_head in range(head_count):
        columns = slice(which_head * HD, (which_head + 1) * HD)
        expos = jnp.where(
            valid_tiles,
            jnp.exp(score_list[which_head] - row_top[:, which_head : which_head + 1]),
            0.0,
        )
        expo_list.append(expos)
        total_list.append(jnp.sum(expos, axis=1))
        weighted_list.append(
            jnp.dot(
                expos.astype(jnp.bfloat16),
                value_block[:, columns],
                preferred_element_type=jnp.float32,
            )
        )
    partial_sums = jnp.concatenate(weighted_list, axis=1)
    partial_totals = jnp.stack(total_list, axis=1)
    weighted, totals = lax.psum((partial_sums, partial_totals), "seq")
    span = weighted.shape[0]
    attended = jnp.where(
        every_row < live_count,
        (weighted.reshape(span, head_count, HD) / totals[:, :, None]).reshape(span, local_width),
        0.0,
    ).astype(jnp.bfloat16)
    own_attended = lax.dynamic_slice_in_dim(attended, first_row, local_rows, 0)
    pooled_part = jnp.dot(own_attended, out_weight, preferred_element_type=jnp.float32)
    pooled_parts = [
        lax.psum_scatter(pooled_part.astype(jnp.bfloat16), "head", scatter_dimension=1, tiled=True)
    ]
    projected = jnp.einsum(
        "rd,cd->rc", cotangent[0], out_weight, preferred_element_type=jnp.float32
    )
    upstream = jnp.where(own_row < live_count, projected, 0.0).astype(jnp.bfloat16)
    upstream_all = lax.all_gather(upstream, "seq", axis=0, tiled=True)
    row_delta = jnp.sum(
        (upstream_all.astype(jnp.float32) * attended.astype(jnp.float32)).reshape(
            total_rows, head_count, HD
        ),
        axis=2,
    )
    query_list = []
    key_list = []
    value_list = []
    for which_head in range(head_count):
        columns = slice(which_head * HD, (which_head + 1) * HD)
        up_head = upstream_all[:, columns]
        weights = expo_list[which_head] / totals[:, which_head : which_head + 1]
        value_list.append(
            jnp.einsum(
                "qt,qc->tc",
                weights.astype(jnp.bfloat16),
                up_head,
                preferred_element_type=jnp.float32,
            )
        )
        grad_prob = jnp.einsum(
            "qc,tc->qt", up_head, value_block[:, columns], preferred_element_type=jnp.float32
        )
        grad_score = (
            weights * (grad_prob - row_delta[:, which_head : which_head + 1]) * factor
        ).astype(jnp.bfloat16)
        query_list.append(
            jnp.dot(grad_score, key_block[:, columns], preferred_element_type=jnp.float32)
        )
        key_list.append(
            jnp.einsum(
                "qt,qc->tc", grad_score, queries[:, columns], preferred_element_type=jnp.float32
            )
        )
    grad_rows = jnp.concatenate(query_list, axis=1)
    key_grads = [jnp.concatenate(key_list, axis=1).astype(jnp.bfloat16)]
    value_grads = [jnp.concatenate(value_list, axis=1).astype(jnp.bfloat16)]
    own_grad = lax.psum_scatter(
        grad_rows.astype(jnp.bfloat16), "seq", scatter_dimension=0, tiled=True
    )
    grad_latents = lax.psum(own_grad, "slide").astype(jnp.float32)
    return (
        jnp.stack(pooled_parts, axis=0),
        grad_latents,
        jnp.stack(key_grads, axis=0),
        jnp.stack(value_grads, axis=0),
    )


def dot_nn(a, b):
    return lax.dot_general(a, b, (((1,), (0,)), ((), ())), preferred_element_type=f32)


def dot_nt(a, b):
    return lax.dot_general(a, b, (((1,), (1,)), ((), ())), preferred_element_type=f32)


def lane_block(index, width):
    return pl.ds(pl.multiple_of(index * width, width), width)


def pack_keys_kernel(n, mask_ref, keys_ref, latents_ref, *rest):
    outs, mask, sems = rest[:n], rest[n], rest[n + 1]
    me = lax.axis_index("seq")
    tiles, rows, width = keys_ref.shape[1], latents_ref.shape[0], outs[0].shape[1]
    sources = [(mask_ref, mask)]
    for d in range(n):
        columns = lane_block(me ^ d, width)
        sources.append((keys_ref.at[0, :, columns], outs[d].at[:tiles, :]))
        sources.append((latents_ref.at[:, columns], outs[d].at[tiles : tiles + rows, :]))
    copies = [
        pltpu.make_async_copy(source, target, sems.at[i])
        for i, (source, target) in enumerate(sources)
    ]
    for copy in copies:
        copy.start()
    copies[0].wait()
    row_id = lax.broadcasted_iota(jnp.int32, (MASK_ROWS, width), 0)
    flags = jnp.zeros((MASK_ROWS, width), f32)
    for block in range(tiles // BLOCK):
        value = jnp.where(mask[0, block] > 0, 1.0, 0.0)
        flags = jnp.where(row_id == block, value, flags)
    for d in range(n):
        outs[d][tiles + rows :, :] = flags.astype(bf16)
    for copy in copies[1:]:
        copy.wait()


def pack_values_kernel(n, count_ref, values_ref, weight_ref, cot_ref, *rest):
    u_outs, v_outs, live_ref = rest[:n], rest[n : 2 * n], rest[2 * n]
    weight, cot, up_ref, sems = rest[2 * n + 1 :]
    me = lax.axis_index("seq")
    width, rows = u_outs[0].shape
    sources = [(weight_ref, weight), (cot_ref.at[0], cot)]
    for d in range(n):
        sources.append((values_ref.at[0, :, lane_block(me ^ d, width)], v_outs[d]))
    copies = [
        pltpu.make_async_copy(source, target, sems.at[i])
        for i, (source, target) in enumerate(sources)
    ]
    for copy in copies:
        copy.start()
    lane_row = lax.broadcasted_iota(jnp.int32, (1, rows), 1)
    for d in range(n):
        source_row = lane_row + (me ^ d) * rows
        live_ref[:, d * rows : (d + 1) * rows] = jnp.where(source_row < count_ref[0], 1.0, 0.0)
    for copy in copies[:2]:
        copy.wait()
    up_ref[...] = dot_nt(weight[...], cot[...]).astype(bf16)
    for d in range(n):
        u_outs[d][...] = up_ref[lane_block(me ^ d, width), :]
    for copy in copies[2:]:
        copy.wait()


def head_mask(h, shape, axis):
    return lax.broadcasted_iota(jnp.int32, shape, axis) // HD == h


def softmax_kernel(n, heads, rows, *refs):
    a_refs = refs[:n]
    expo_ref, total_ref, keys_t_ref, score_ref = refs[n:]
    width = heads * HD
    tiles = expo_ref.shape[2]
    total_rows = n * rows
    per_block = tiles // BLOCK
    scale = HD ** (-0.5) * math.log2(math.e)
    queries = jnp.concatenate([a_refs[d][tiles : tiles + rows, :] for d in range(n)], axis=0)
    queries_t = queries.astype(f32).T.astype(bf16)
    valid = []
    for d in range(n):
        flags = a_refs[d][tiles + rows :, :].astype(f32)
        for j in range(per_block):
            valid.append(
                jnp.concatenate([flags[j : j + 1, :]] * (total_rows // width), axis=1) > 0.5
            )
    for h in range(heads):
        top = jnp.full((1, total_rows), masked_score, f32)
        query_h = jnp.where(
            head_mask(h, (width, total_rows), 0), queries_t, jnp.zeros_like(queries_t)
        )
        for d in range(n):
            scored = dot_nn(a_refs[d][:tiles, :], query_h)
            score_ref[d] = scored
            for j in range(per_block):
                block_top = jnp.max(scored[j * BLOCK : (j + 1) * BLOCK], axis=0, keepdims=True)
                top = jnp.maximum(top, jnp.where(valid[d * per_block + j], block_top, masked_score))
        total = jnp.zeros((1, total_rows), f32)
        for d in range(n):
            for j in range(per_block):
                part = slice(j * BLOCK, (j + 1) * BLOCK)
                expos = jnp.where(
                    valid[d * per_block + j], jnp.exp2((score_ref[d, part, :] - top) * scale), 0.0
                )
                total = total + jnp.sum(expos, axis=0, keepdims=True)
                expo_ref[h, d, part, :] = expos.astype(bf16)
        total_ref[h] = total
    for d in range(n):
        keys_t_ref[d] = a_refs[d][:tiles, :].astype(f32).T.astype(bf16)


def value_grads_kernel(n, heads, live_ref, expo_ref, total_ref, *refs):
    u_refs, up_ref, outs = refs[:n], refs[n], refs[n + 1 :]
    factor = HD ** (-0.5)
    upstream_t = jnp.concatenate([u_refs[d][...] for d in range(n)], axis=1)
    live = live_ref[...] > 0.5
    up_scaled_t = jnp.concatenate(
        [
            jnp.where(
                live, upstream_t[h * HD : (h + 1) * HD, :].astype(f32) * (factor / total_ref[h]), 0.0
            )
            for h in range(heads)
        ],
        axis=0,
    )
    up_ref[...] = up_scaled_t.astype(bf16)
    up_scaled = up_scaled_t.T
    up_heads = [
        jnp.where(head_mask(h, up_scaled.shape, 1), up_scaled, 0.0).astype(bf16)
        for h in range(heads)
    ]
    for d in range(n):
        value_grad = dot_nn(expo_ref[0, d], up_heads[0])
        for h in range(1, heads):
            value_grad = value_grad + dot_nn(expo_ref[h, d], up_heads[h])
        outs[d][...] = (value_grad * (1.0 / factor)).astype(bf16)


def key_grads_kernel(n, heads, rows, live_ref, expo_ref, total_ref, up_ref, keys_t_ref, *refs):
    a_refs, v_refs = refs[:n], refs[n : 2 * n]
    outs, query_grad_ref = refs[2 * n : 3 * n], refs[3 * n]
    width = heads * HD
    tiles = v_refs[0].shape[0]
    total_rows = n * rows
    live = live_ref[...] > 0.5
    queries = jnp.concatenate([a_refs[d][tiles : tiles + rows, :] for d in range(n)], axis=0)
    up_scaled_t = up_ref[...]
    values_t = [v_refs[d][...].astype(f32).T.astype(bf16) for d in range(n)]
    attended_list = []
    delta_list = []
    for h in range(heads):
        own_rows = slice(h * HD, (h + 1) * HD)
        weighted = dot_nn(values_t[0][own_rows, :], expo_ref[h, 0])
        for d in range(1, n):
            weighted = weighted + dot_nn(values_t[d][own_rows, :], expo_ref[h, d])
        attended_h = jnp.where(live, weighted / total_ref[h], 0.0).astype(bf16)
        delta_list.append(
            jnp.sum(
                up_scaled_t[own_rows, :].astype(f32) * attended_h.astype(f32),
                axis=0,
                keepdims=True,
            )
        )
        attended_list.append(attended_h)
    attended = jnp.concatenate(attended_list, axis=0)
    zero_rows = jnp.zeros_like(queries)
    zero_cols = jnp.zeros_like(up_scaled_t)
    query_heads = [jnp.where(head_mask(h, queries.shape, 1), queries, zero_rows) for h in range(heads)]
    up_heads_t = [
        jnp.where(head_mask(h, up_scaled_t.shape, 0), up_scaled_t, zero_cols) for h in range(heads)
    ]
    query_grad = [jnp.zeros((HD, total_rows), f32) for _ in range(heads)]
    for d in range(n):
        key_grad = jnp.zeros((tiles, width), f32)
        for h in range(heads):
            grad_prob = dot_nn(v_refs[d][...], up_heads_t[h])
            grad_score = (expo_ref[h, d].astype(f32) * (grad_prob - delta_list[h])).astype(bf16)
            key_grad = key_grad + dot_nn(grad_score, query_heads[h])
            query_grad[h] = query_grad[h] + dot_nn(
                keys_t_ref[d, h * HD : (h + 1) * HD, :], grad_score
            )
        outs[d][:tiles, :] = key_grad.astype(bf16)
        outs[d][tiles:, :] = attended[:, d * rows : (d + 1) * rows]
    query_grad_ref[...] = jnp.concatenate(query_grad, axis=0).astype(bf16)


def values_home_kernel(n, *refs):
    c_refs, value_grad_ref = refs[:n], refs[n]
    me = lax.axis_index("seq")
    width = c_refs[0].shape[1]
    for d in range(n):
        value_grad_ref[0, :, lane_block((me ^ d), width)] = c_refs[d][...]


def pool_kernel(n, weight_ref, *refs):
    k_refs = refs[:n]
    kept_ref, sent_ref = refs[n : n + 2]
    me, side = lax.axis_index("seq"), lax.axis_index("head")
    width = k_refs[0].shape[1]
    tiles = k_refs[0].shape[0] - width
    half = kept_ref.shape[1]
    kept = jnp.zeros(kept_ref.shape, f32)
    sent = jnp.zeros(sent_ref.shape, f32)
    for d in range(n):
        owner = (me ^ d)
        attended = k_refs[d][tiles:, :].astype(f32).T.astype(bf16)
        inputs = lane_block(owner, width)
        kept = kept + dot_nn(attended, weight_ref[inputs, lane_block(side, half)])
        sent = sent + dot_nn(attended, weight_ref[inputs, lane_block(1 - side, half)])
    kept_ref[...] = kept
    sent_ref[...] = sent.astype(bf16)


def keys_home_kernel(n, *refs):
    k_refs, key_grad_ref = refs[:n], refs[n]
    me = lax.axis_index("seq")
    width = k_refs[0].shape[1]
    tiles = key_grad_ref.shape[1]
    for d in range(n):
        key_grad_ref[0, :, lane_block(me ^ d, width)] = k_refs[d][:tiles, :]


def join_kernel(n, own_ref, other_ref, *outs):
    rows = outs[0].shape[1]
    both = (own_ref[...].astype(f32) + other_ref[...].astype(f32)).astype(bf16)
    for d in range(n):
        outs[d][...] = both[:, d * rows : (d + 1) * rows]


def last_kernel(n, kept_ref, came_ref, *refs):
    g_refs, latent_grad_ref, pooled_ref = refs[:n], refs[n], refs[n + 1]
    me = lax.axis_index("seq")
    width = g_refs[0].shape[0]
    for d in range(n):
        columns = lane_block((me ^ d), width)
        latent_grad_ref[:, columns] = g_refs[d][...].astype(f32).T
    pooled_ref[0] = (kept_ref[...] + came_ref[...].astype(f32)).astype(bf16)


SMEM = pl.BlockSpec(memory_space=pltpu.SMEM)
HBM = pl.BlockSpec(memory_space=pltpu.HBM)
VMEM = pl.BlockSpec(memory_space=pltpu.VMEM)


def call(kernel, out_shape, operands, flops, scratch=(), grant=8, spaces=None):
    moved = sum(x.size * x.dtype.itemsize for x in operands)
    moved += sum(math.prod(x.shape) * x.dtype.itemsize for x in out_shape)
    return pl.pallas_call(
        kernel,
        out_shape=out_shape,
        in_specs=spaces or [VMEM] * len(operands),
        out_specs=[VMEM] * len(out_shape),
        scratch_shapes=list(scratch),
        cost_estimate=pl.CostEstimate(flops=int(flops), bytes_accessed=moved, transcendentals=0),
        compiler_params=pltpu.CompilerParams(vmem_limit_bytes=grant * 1024 * 1024),
    )(*operands)


def exchanged_body(n, sides, latents, tile_keys, tile_values, tile_mask, latent_counts, out_weight, cotangent):
    rows, local_width = latents.shape
    tiles = tile_keys.shape[1]
    out_width = out_weight.shape[1]
    heads = local_width // HD // n
    width = heads * HD
    total_rows = n * rows
    sds = jax.ShapeDtypeStruct
    product = 2 * total_rows * n * tiles * width

    def spread(pieces):
        came = {0: pieces[0]}
        for d in offsets(n):
            came[d] = lax.ppermute(pieces[d], "seq", [(i, i ^ d) for i in range(n)])
        return [came[d] for d in range(n)]

    def in_hbm(*arrays):
        return tuple(pltpu.with_memory_space_constraint(x, pltpu.HBM) for x in arrays)

    packed = call(
        functools.partial(pack_keys_kernel, n),
        [sds((tiles + rows + MASK_ROWS, width), bf16)] * n,
        in_hbm(tile_mask, tile_keys, latents),
        1e6,
        [pltpu.SMEM(tile_mask.shape, jnp.int32), pltpu.SemaphoreType.DMA((1 + 2 * n,))],
        spaces=[HBM] * 3,
    )
    a_list = spread(packed)
    *packed, live = call(
        functools.partial(pack_values_kernel, n),
        [sds((width, rows), bf16)] * n
        + [sds((tiles, width), bf16)] * n
        + [sds((1, total_rows), f32)],
        (latent_counts, *in_hbm(tile_values, out_weight, cotangent)),
        2 * rows * local_width * out_width,
        [
            pltpu.VMEM(out_weight.shape, bf16),
            pltpu.VMEM(cotangent.shape[1:], bf16),
            pltpu.VMEM((local_width, rows), bf16),
            pltpu.SemaphoreType.DMA((2 + n,)),
        ],
        spaces=[SMEM] + [HBM] * 3,
    )
    u_list = spread(packed[:n])
    v_list = spread(packed[n:])
    expos, totals, keys_t = call(
        functools.partial(softmax_kernel, n, heads, rows),
        [
            sds((heads, n, tiles, total_rows), bf16),
            sds((heads, 1, total_rows), f32),
            sds((n, width, tiles), bf16),
        ],
        a_list,
        product,
        [pltpu.VMEM((n, tiles, total_rows), f32)],
        16,
    )
    up_scaled, *c_out = call(
        functools.partial(value_grads_kernel, n, heads),
        [sds((width, total_rows), bf16)] + [sds((tiles, width), bf16)] * n,
        (live, expos, totals, *u_list),
        product,
        (),
        16,
    )
    c_list = spread(c_out)
    *k_out, query_grad = call(
        functools.partial(key_grads_kernel, n, heads, rows),
        [sds((tiles + width, width), bf16)] * n + [sds((width, total_rows), bf16)],
        (live, expos, totals, up_scaled, keys_t, *a_list, *v_list),
        4 * product,
        (),
        16,
    )
    other_sum = None
    for step in range(1, sides):
        came = lax.ppermute(query_grad, "slide", [(i, (i + step) % sides) for i in range(sides)])
        other_sum = came if other_sum is None else other_sum.astype(f32) + came.astype(f32)
    k_list = spread(k_out)
    joined = call(
        functools.partial(join_kernel, n),
        [sds((width, rows), bf16)] * n,
        (query_grad, other_sum),
        1e6,
    )
    g_list = spread(joined)
    (value_grads,) = call(
        functools.partial(values_home_kernel, n), [sds(tile_values.shape, bf16)], c_list, 1e6
    )
    kept, sent = call(
        functools.partial(pool_kernel, n),
        [
            sds((rows, out_width // 2), f32),
            sds((rows, out_width // 2), bf16),
        ],
        (out_weight, *k_list),
        2 * rows * local_width * out_width,
    )
    came = lax.ppermute(sent, "head", [(0, 1), (1, 0)])
    (key_grads,) = call(
        functools.partial(keys_home_kernel, n), [sds(tile_keys.shape, bf16)], k_list, 1e6
    )
    latent_grads, pooled = call(
        functools.partial(last_kernel, n),
        [sds(latents.shape, f32), sds((1, rows, out_width // 2), bf16)],
        (kept, came, *g_list),
        1e6,
    )
    return pooled, latent_grads, key_grads, value_grads


def offsets(n):
    return [*range(n // 2, n), *range(n // 2 - 1, 0, -1)]


def solution(mesh):
    placed = (
        P(("groups", "seq"), "head"),
        P(("groups", "slide"), "seq", "head"),
        P(("groups", "slide"), "seq", "head"),
        P(("groups", "slide"), "seq"),
        P(("groups", "slide")),
        P("head", None),
        P(("groups", "slide"), "seq", None),
    )
    n, sides = mesh.shape["seq"], mesh.shape["slide"]

    def body(latents, tile_keys, *rest):
        rows, local_width = latents.shape
        tiles = tile_keys.shape[1]
        fits = (
            mesh.shape["head"] == 2
            and sides > 1
            and local_width % (n * LANES) == 0
            and local_width // n == rows
            and tiles % BLOCK == 0
            and tiles // BLOCK <= MASK_ROWS
            and n >= 4
            and n & (n - 1) == 0
        )
        if fits:
            return exchanged_body(n, sides, latents, tile_keys, *rest)
        return gathered_body(latents, tile_keys, *rest)

    return jax.shard_map(
        body,
        mesh=mesh,
        in_specs=placed,
        out_specs=(
            P(("groups", "slide"), "seq", "head"),
            P(("groups", "seq"), "head"),
            P(("groups", "slide"), "seq", "head"),
            P(("groups", "slide"), "seq", "head"),
        ),
        check_vma=False,
    )
```
